32 devices in a mesh: grp: 16 (over z, x, core), fsdp: 2 (over y).
Axes of the slice: x: 2, y: 2, z: 4, core: 2. Of those that a mesh axis runs over, the one named last changes fastest.
Arguments:
- normalized_inputs: bfloat16 [4096, 2048], P(('grp', 'fsdp')), may hold values from -6 to 6
- output_sensitivity: bfloat16 [4096, 512], P(('grp', 'fsdp')), may hold values from -6 to 6
- projection_weights: bfloat16 [2048, 512], P('fsdp'), may hold values from -0.25 to 0.25
- completion_mask: int32 [16], replicated, may hold values 0 or 1
- replica_partition_list: int32 [16], replicated, may hold values from 0 to 3, as said below
Outputs:
- input_grad: bfloat16 [4096, 2048], P(('grp', 'fsdp'))
- weight_grad: float32 [2048, 512], P(('grp', 'fsdp'))
The draws below stay inside these ranges and needn't reach their ends.
Inputs may be any that keep to these rules, and one draw needn't show every extreme that they name: `replica_partition_list`: each of the 4 block numbers is named by exactly 4 groups.
All inputs are finite; a program needn't handle non-finite values.
Results may differ from the reference program's by a relative error of at most 0.001.
Values may be sent and summed in bfloat16 or wider, within the bound.
A program may use at most 64 MiB of HBM per device.

```python
import jax
import jax.numpy as jnp
from jax import lax

D = 2048
KVW = 512
REP = 4
REPLICA_SETS = 16
TOKENS = 4096


def draw_replica_partition_list(key, part):
    return (jax.random.permutation(key, REPLICA_SETS) // REP).astype(jnp.int32)


def plant(values, rng, smallest, largest):
    shape = values.shape
    spot = [jax.random.randint(jax.random.fold_in(rng, axis), (), 0, shape[axis]) for axis in range(len(shape))]
    values = values.at[tuple(spot)].set(smallest)
    longest = shape.index(max(shape))
    spot[longest] = (spot[longest] + 1) % shape[longest]
    return values.at[tuple(spot)].set(largest)


def raised(drawn, stream_key, source, target, parts, factor):
    owner, partner = [(jnp.arange(drawn.shape[dim]) // (drawn.shape[dim] // parts)).reshape([-1 if axis == dim else 1 for axis in range(drawn.ndim)]) for dim in (source, target)]
    chosen = jax.random.permutation(stream_key, parts)[partner]
    strong = (owner == chosen) | (owner == (partner + parts // 2) % parts)
    return jnp.where(strong, factor * drawn, drawn)


def block_scale(key, extent, pieces, low, top_value):
    level, own = 1.0, jax.random.fold_in(key, 6)
    for dim, blocks in pieces:
        steps = jnp.exp(jax.random.uniform(jax.random.fold_in(own, dim), (blocks,), jnp.float32, low / len(pieces), top_value / len(pieces)))
        level = level * jnp.repeat(steps, extent[dim] // blocks).reshape([-1 if axis == dim else 1 for axis in range(len(extent))])
    return level


def noise(rng, dims, width, reach, cuts=(), dtype=jnp.bfloat16):
    values = width * jax.random.normal(rng, dims, jnp.float32)
    if cuts:
        values = values * block_scale(rng, dims, cuts, -0.22, 0.18)
    return jnp.clip(values, -reach, reach).astype(dtype)


def gaussian_with(stream_key, extent, spread, reach, cuts, heavy, held_as=jnp.bfloat16):
    result = spread * jax.random.normal(stream_key, extent, jnp.float32)
    if cuts:
        result = result * block_scale(stream_key, extent, cuts, -0.22, 0.18)
    return jnp.clip(raised(result, jax.random.fold_in(stream_key, 3), *heavy), -reach, reach).astype(held_as)


def setup_inputs(seed: int = 0) -> dict:
    seeds = jax.random.split(jax.random.key(seed), 6)
    return {
        "normalized_inputs": gaussian_with(seeds[0], (TOKENS, D), 1.0, 6.0, ((0, 32),), (0, 1, 32, 2.75)),
        "output_sensitivity": noise(seeds[1], (TOKENS, KVW), 1.0, 6.0, ((0, 32),)),
        "projection_weights": noise(seeds[2], (D, KVW), KVW ** -0.5, 0.25, ((0, 2),)),
        "completion_mask": plant((jax.random.randint(seeds[3], (REPLICA_SETS,), 0, 4) < 3).astype(jnp.int32), jax.random.fold_in(seeds[3], 1), 0, 1),
        "replica_partition_list": draw_replica_partition_list(jax.random.fold_in(seeds[5], 71), 0),
    }


def reference(normalized_inputs, output_sensitivity, projection_weights, completion_mask, replica_partition_list):
    replica_amount = completion_mask.shape[0]
    corresponding_piece = (replica_partition_list[:, None] == replica_partition_list[None, :]).astype(jnp.int32)
    finisher_tally = jnp.sum(corresponding_piece * completion_mask[None, :], axis=1).astype(jnp.int32)
    finished_indicator = completion_mask.astype(jnp.float32)
    decode_sum = finished_indicator / (finisher_tally.astype(jnp.float32) + 1.0 - finished_indicator)
    input_grad = jnp.dot(output_sensitivity, projection_weights.T, preferred_element_type=jnp.float32).astype(jnp.bfloat16)
    model_width = normalized_inputs.shape[1]
    value_width = output_sensitivity.shape[1]
    group_rows = normalized_inputs.shape[0] // replica_amount
    acts_grouped = normalized_inputs.reshape(replica_amount, group_rows, model_width)
    cots_grouped = output_sensitivity.reshape(replica_amount, group_rows, value_width)

    def accumulate(running, pieces_in):
        acts_here, cots_here, scale_here = pieces_in
        product = lax.dot_general(acts_here, cots_here, (((0,), (0,)), ((), ())), preferred_element_type=jnp.float32)
        return running + scale_here * product, None

    initial = jnp.zeros((model_width, value_width), jnp.float32)
    weight_grad, _ = lax.scan(accumulate, initial, (acts_grouped, cots_grouped, decode_sum))
    return input_grad, weight_grad
```

```python
import functools

import jax
import jax.numpy as jnp
from jax import lax
from jax.experimental import pallas as pl
from jax.experimental.pallas import tpu as pltpu
from jax.sharding import PartitionSpec as P

MESH = pl.DeviceIdType.MESH
CORES = 2
WIDE = 2
STEPS = 32766.0
TINY = 1e-33


def collective_shards(
    normalized_inputs,
    output_sensitivity,
    projection_weights,
    completion_mask,
    replica_partition_list,
):
    replica_index = lax.axis_index("grp")
    selected_replica = lax.iota(jnp.int32, completion_mask.shape[0]) == replica_index
    assigned_piece = jnp.sum(jnp.where(selected_replica, replica_partition_list, 0))
    finished_indicator = jnp.sum(jnp.where(selected_replica, completion_mask, 0))
    finisher_tally = jnp.sum(
        jnp.where(replica_partition_list == assigned_piece, completion_mask, 0)
    )
    living_float = finished_indicator.astype(jnp.float32)
    decode_sum = living_float / (finisher_tally.astype(jnp.float32) + 1.0 - living_float)
    tokens_here = normalized_inputs.shape[0]
    model_width = normalized_inputs.shape[1]
    inner_size = lax.axis_size("fsdp")
    outer_size = lax.axis_size("grp")
    input_grad = lax.dot_general(
        output_sensitivity,
        lax.all_gather(projection_weights, "fsdp", axis=0, tiled=True),
        (((1,), (1,)), ((), ())),
        preferred_element_type=jnp.float32,
    ).astype(jnp.bfloat16)
    owner_rows = model_width // (outer_size * inner_size)
    reordered = normalized_inputs.reshape(tokens_here, outer_size, inner_size, owner_rows)
    reordered = reordered.transpose(0, 2, 1, 3).reshape(tokens_here, model_width)
    column_block = lax.all_to_all(reordered, "fsdp", split_axis=1, concat_axis=0, tiled=True)
    group_block = lax.dot_general(
        column_block,
        lax.all_gather(output_sensitivity, "fsdp", axis=0, tiled=True),
        (((0,), (0,)), ((), ())),
        preferred_element_type=jnp.float32,
    )
    weight_grad = lax.psum_scatter(decode_sum * group_block, "grp", scatter_dimension=0, tiled=True)
    return (input_grad, weight_grad)


def encode(value):
    top = jnp.maximum(jnp.max(jnp.abs(value), axis=0, keepdims=True), TINY)
    coded = jnp.round(value * (STEPS / top)).astype(jnp.int32).astype(jnp.int16)
    return coded, top * (1.0 / STEPS)


def decoded(coded, step):
    return coded.astype(jnp.int32).astype(jnp.float32) * step


def kernel(
    deep,
    mask_hbm, list_hbm, x_hbm, s_hbm, w_hbm,
    ig_ref, wg_ref,
    mask_ref, list_ref,
    x_v, s_v, w_v, tx, rx, own_part, px_send, px_scale, px_recv, px_rscale,
    q, q_send, q_scale, zr, zr_scale, ig_send,
    load_sem, s_send_sem, s_recv_sem, x_send_sem, x_recv_sem,
    px_send_sem, px_recv_sem, z_send_sem, z_recv_sem, ig_send_sem, ig_recv_sem, hello,
):
    grp = lax.axis_index("grp")
    y = lax.axis_index("fsdp")
    core = lax.rem(grp, CORES)
    wide = lax.rem(grp // CORES, WIDE)
    z = grp // (CORES * WIDE)
    oy, oc = 1 - y, 1 - core
    tokens = s_hbm.shape[0]
    groups = mask_ref.shape[0]
    rows = wg_ref.shape[0]
    half = w_hbm.shape[0]
    part_tokens = tokens // 2

    def at(zz, xx, cc, yy):
        return ((zz * WIDE + xx) * CORES + cc, yy)

    def remote(src, dst, send, recv, device):
        return pltpu.make_async_remote_copy(
            src_ref=src, dst_ref=dst, send_sem=send, recv_sem=recv,
            device_id=device, device_id_type=MESH,
        )

    y_peer = at(z, wide, core, oy)
    y_cross = at(z, wide, oc, oy)
    sibling = at(z, wide, oc, y)
    x_peer = at(z, 1 - wide, core, y)
    below = at(lax.rem(z + deep - 1, deep), wide, core, y)
    above = at(lax.rem(z + 1, deep), wide, core, y)
    me = core * 2 + y
    from_y = core * 2 + oy
    from_cross = oc * 2 + oy
    from_sib = oc * 2 + y

    barrier = pltpu.get_barrier_semaphore()
    partners = [y_peer, y_cross, sibling, x_peer]
    for partner in partners:
        pl.semaphore_signal(barrier, inc=1, device_id=partner, device_id_type=MESH)

    @pl.when(z > 0)
    def _():
        pl.semaphore_signal(barrier, inc=1, device_id=below, device_id_type=MESH)

    @pl.when(z < deep - 1)
    def _():
        pl.semaphore_signal(barrier, inc=1, device_id=above, device_id_type=MESH)

    load_x = pltpu.make_async_copy(x_hbm, x_v, load_sem.at[0])
    load_s = pltpu.make_async_copy(s_hbm, s_v.at[me], load_sem.at[1])
    load_w = pltpu.make_async_copy(w_hbm, w_v, load_sem.at[2])
    load_mask = pltpu.make_async_copy(mask_hbm, mask_ref, load_sem.at[3])
    load_list = pltpu.make_async_copy(list_hbm, list_ref, load_sem.at[4])
    loads = [load_x, load_s, load_w, load_mask, load_list]
    for load in loads:
        load.start()

    first, second = pl.ds(0, part_tokens), pl.ds(part_tokens, part_tokens)
    s_y = remote(s_hbm.at[first], s_v.at[me, first], s_send_sem.at[0], s_recv_sem.at[0], y_peer)
    s_cross = remote(s_hbm.at[second], s_v.at[me, second], s_send_sem.at[1], s_recv_sem.at[1], y_cross)
    s_sib = remote(s_hbm, s_v.at[me], s_send_sem.at[2], s_recv_sem.at[2], sibling)
    forward_y = remote(
        s_v.at[from_y, first], s_v.at[from_y, first], s_send_sem.at[3], s_recv_sem.at[3], sibling
    )
    forward_cross = remote(
        s_v.at[from_cross, second], s_v.at[from_cross, second], s_send_sem.at[4], s_recv_sem.at[4], sibling
    )

    @pl.when(jnp.logical_and(z > 0, z < deep - 1))
    def _():
        pl.semaphore_wait(barrier, len(partners) + 2)

    @pl.when(jnp.logical_or(z == 0, z == deep - 1))
    def _():
        pl.semaphore_wait(barrier, len(partners) + 1)

    s_y.start()
    s_cross.start()
    s_sib.start()

    @pl.when(z == deep - 2)
    def _():
        pl.semaphore_signal(hello.at[0], inc=1, device_id=below, device_id_type=MESH)

    @pl.when(z == 1)
    def _():
        pl.semaphore_signal(hello.at[1], inc=1, device_id=above, device_id_type=MESH)

    span = WIDE * CORES * 2 * rows

    def plane(n):
        if n == deep - 1:
            return z
        return jnp.where(z == 0, deep - 1 - n, jnp.where(n < z, n, n + 1))

    def turn(n):
        part = x_v[:, pl.ds(pl.multiple_of(plane(n) * span, span), span)].T
        for xx in range(WIDE):
            for cy in range(CORES * 2):
                start = (xx * CORES * 2 + cy) * rows
                tx[n, cy, xx * rows:(xx + 1) * rows, :] = part[start:start + rows, :]

    load_x.wait()
    x_copies = []
    for n in range(deep):
        turn(n)
        p = plane(n)
        copies = []
        for slot, (device, there) in enumerate(
            ((y_peer, from_y), (y_cross, from_cross), (sibling, from_sib))
        ):
            copy = remote(
                tx.at[n, there], rx.at[n, me], x_send_sem.at[n, slot], x_recv_sem.at[n, slot], device
            )
            copy.start()
            copies.append(copy)
        x_copies.append(copies)
        rx[n, me] = tx[n, me]

    load_mask.wait()
    load_list.wait()
    scales = []
    for cc in range(CORES):
        here = (z * WIDE + wide) * CORES + cc
        mine = list_ref[here]
        tally = jnp.int32(0)
        for h in range(groups):
            tally = tally + jnp.where(list_ref[h] == mine, mask_ref[h], 0)
        done = jnp.full((1, wg_ref.shape[1]), mask_ref[here], jnp.int32).astype(jnp.float32)
        total = jnp.full((1, wg_ref.shape[1]), tally, jnp.int32).astype(jnp.float32)
        scales.append(done / (total + 1.0 - done))

    load_s.wait()
    load_w.wait()

    def grad(s_block):
        return lax.dot_general(
            s_block, w_v[...], (((1,), (1,)), ((), ())), preferred_element_type=jnp.float32
        ).astype(jnp.bfloat16)

    own_columns = pl.ds(pl.multiple_of(y * half, half), half)
    ig_ref[:, own_columns] = grad(s_v[me])

    s_y.wait_recv()
    forward_y.start()
    s_cross.wait_recv()
    forward_cross.start()
    ig_send[...] = grad(jnp.concatenate([s_v[from_y, first], s_v[from_cross, second]], axis=0))
    ig_y = remote(ig_send.at[first], ig_ref.at[first, own_columns], ig_send_sem.at[0], ig_recv_sem.at[0], y_peer)
    ig_cross = remote(
        ig_send.at[second], ig_ref.at[second, own_columns], ig_send_sem.at[1], ig_recv_sem.at[1], y_cross
    )
    ig_y.start()
    ig_cross.start()

    @pl.when(jnp.logical_and(z > 0, z < deep - 2))
    def _():
        pl.semaphore_wait(hello.at[0], 1)
        pl.semaphore_signal(hello.at[0], inc=1, device_id=below, device_id_type=MESH)

    @pl.when(jnp.logical_and(z > 1, z < deep - 1))
    def _():
        pl.semaphore_wait(hello.at[1], 1)
        pl.semaphore_signal(hello.at[1], inc=1, device_id=above, device_id_type=MESH)

    s_sib.wait_recv()
    forward_y.wait_recv()
    forward_cross.wait_recv()

    px_copies, z_copies = {}, {}

    def partial(n):
        for copy in x_copies[n]:
            copy.wait_recv()
        total = None
        for cc in range(CORES):
            left = jnp.concatenate([rx[n, cc * 2], rx[n, cc * 2 + 1]], axis=1)
            right = s_v[cc * 2:cc * 2 + 2].reshape(2 * tokens, s_v.shape[2])
            product = scales[cc] * jnp.dot(left, right, preferred_element_type=jnp.float32)
            total = product if total is None else total + product
        own_part[n, 0] = total[:rows]
        own_part[n, 1] = total[rows:]
        coded, scale = encode(own_part[n, 1 - wide])
        px_send[n] = coded
        px_scale[n] = scale

    def send_x(n):
        copies = [
            remote(px_send.at[n], px_recv.at[n], px_send_sem.at[n, 0], px_recv_sem.at[n, 0], x_peer),
            remote(px_scale.at[n], px_rscale.at[n], px_send_sem.at[n, 1], px_recv_sem.at[n, 1], x_peer),
        ]
        for copy in copies:
            copy.start()
        px_copies[n] = copies

    def gather_x(n):
        for copy in px_copies[n]:
            copy.wait_recv()
        value = own_part[n, wide] + decoded(px_recv[n], px_rscale[n])
        if n < deep - 1:
            coded, scale = encode(value)
            q_send[n] = coded
            q_scale[n] = scale
            there = at(plane(n), wide, core, y)
            copies = [
                remote(q_send.at[n], zr.at[z], z_send_sem.at[n, 0], z_recv_sem.at[z, 0], there),
                remote(q_scale.at[n], zr_scale.at[z], z_send_sem.at[n, 1], z_recv_sem.at[z, 1], there),
            ]
            for copy in copies:
                copy.start()
            z_copies[n] = copies
        else:
            q[...] = value

    for n in range(deep):
        partial(n)
        send_x(n)
        if n == 1:
            @pl.when(z == 0)
            def _():
                pl.semaphore_wait(hello.at[0], 1)

            @pl.when(z == deep - 1)
            def _():
                pl.semaphore_wait(hello.at[1], 1)
        if n:
            gather_x(n - 1)
    gather_x(deep - 1)

    total = q[...]
    for n in range(deep - 1):
        source = jnp.where(n < z, n, n + 1)
        for piece, part in enumerate((zr, zr_scale)):
            remote(
                part.at[source], part.at[source], z_send_sem.at[n, piece], z_recv_sem.at[source, piece], sibling
            ).wait_recv()
        total = total + decoded(zr[source], zr_scale[source])
    wg_ref[...] = total

    ig_y.wait_recv()
    ig_cross.wait_recv()

    for copy in (s_y, s_cross, s_sib, forward_y, forward_cross, ig_y, ig_cross):
        copy.wait_send()
    for group in (x_copies, px_copies.values(), z_copies.values()):
        for copies in group:
            for copy in copies:
                copy.wait_send()


def kernel_shards(deep, rows, x, s, w, mask, plist):
    tokens, width = x.shape
    values = s.shape[1]
    f32, bf16, i16 = jnp.float32, jnp.bfloat16, jnp.int16
    dma = pltpu.SemaphoreType.DMA
    anywhere = pl.BlockSpec(memory_space=pl.ANY)
    wide_rows = WIDE * rows
    return pl.pallas_call(
        functools.partial(kernel, deep),
        out_shape=(
            pltpu.VMEM((tokens, width), bf16),
            pltpu.VMEM((rows, values), f32),
        ),
        in_specs=[anywhere] * 5,
        out_specs=(pl.BlockSpec(memory_space=pltpu.VMEM),) * 2,
        scratch_shapes=[
            pltpu.SMEM(mask.shape, jnp.int32),
            pltpu.SMEM(plist.shape, jnp.int32),
            pltpu.VMEM((tokens, width), bf16),
            pltpu.VMEM((CORES * 2, tokens, values), bf16),
            pltpu.VMEM(w.shape, bf16),
            pltpu.VMEM((deep, CORES * 2, wide_rows, tokens), bf16),
            pltpu.VMEM((deep, CORES * 2, wide_rows, tokens), bf16),
            pltpu.VMEM((deep, WIDE, rows, values), f32),
            pltpu.VMEM((deep, rows, values), i16),
            pltpu.VMEM((deep, 1, values), f32),
            pltpu.VMEM((deep, rows, values), i16),
            pltpu.VMEM((deep, 1, values), f32),
            pltpu.VMEM((rows, values), f32),
            pltpu.VMEM((deep, rows, values), i16),
            pltpu.VMEM((deep, 1, values), f32),
            pltpu.VMEM((deep, rows, values), i16),
            pltpu.VMEM((deep, 1, values), f32),
            pltpu.VMEM((tokens, w.shape[0]), bf16),
            dma((5,)), dma((5,)), dma((5,)), dma((deep, 3)), dma((deep, 3)),
            dma((deep, 2)), dma((deep, 2)), dma((deep, 2)), dma((deep, 2)), dma((2,)), dma((2,)),
            pltpu.SemaphoreType.REGULAR((2,)),
        ],
        compiler_params=pltpu.CompilerParams(collective_id=0, has_side_effects=True),
    )(mask, plist, x, s, w)


def solution(mesh):
    outer, inner = mesh.shape["grp"], mesh.shape["fsdp"]

    def shards(x, s, w, mask, plist):
        rows = x.shape[1] // (outer * inner)
        if inner == 2 and outer % (CORES * WIDE) == 0 and outer // (CORES * WIDE) >= 4 and rows % 16 == 0 and x.shape[0] % 128 == 0:
            return tuple(kernel_shards(outer // (CORES * WIDE), rows, x, s, w, mask, plist))
        return collective_shards(x, s, w, mask, plist)

    in_specs = (P(("grp", "fsdp"), None), P(("grp", "fsdp"), None), P("fsdp", None), P(), P())
    out_specs = (P(("grp", "fsdp"), None), P(("grp", "fsdp"), None))
    return jax.shard_map(shards, mesh=mesh, in_specs=in_specs, out_specs=out_specs, check_vma=False)
```

```python
import functools

import jax
import jax.numpy as jnp
from jax import lax
from jax.experimental import pallas as pl
from jax.experimental.pallas import tpu as pltpu
from jax.sharding import PartitionSpec as P

MESH = pl.DeviceIdType.MESH
CORES = 2
WIDE = 2
HALVES = 2
LAG = 2
SMALL = 1 << 20
STEPS = 32766.0
TINY = 1e-33


def collective_shards(
    normalized_inputs,
    output_sensitivity,
    projection_weights,
    completion_mask,
    replica_partition_list,
):
    replica_index = lax.axis_index("grp")
    selected_replica = lax.iota(jnp.int32, completion_mask.shape[0]) == replica_index
    assigned_piece = jnp.sum(jnp.where(selected_replica, replica_partition_list, 0))
    finished_indicator = jnp.sum(jnp.where(selected_replica, completion_mask, 0))
    finisher_tally = jnp.sum(
        jnp.where(replica_partition_list == assigned_piece, completion_mask, 0)
    )
    living_float = finished_indicator.astype(jnp.float32)
    decode_sum = living_float / (finisher_tally.astype(jnp.float32) + 1.0 - living_float)
    tokens_here = normalized_inputs.shape[0]
    model_width = normalized_inputs.shape[1]
    inner_size = lax.axis_size("fsdp")
    outer_size = lax.axis_size("grp")
    input_grad = lax.dot_general(
        output_sensitivity,
        lax.all_gather(projection_weights, "fsdp", axis=0, tiled=True),
        (((1,), (1,)), ((), ())),
        preferred_element_type=jnp.float32,
    ).astype(jnp.bfloat16)
    owner_rows = model_width // (outer_size * inner_size)
    reordered = normalized_inputs.reshape(tokens_here, outer_size, inner_size, owner_rows)
    reordered = reordered.transpose(0, 2, 1, 3).reshape(tokens_here, model_width)
    column_block = lax.all_to_all(reordered, "fsdp", split_axis=1, concat_axis=0, tiled=True)
    group_block = lax.dot_general(
        column_block,
        lax.all_gather(output_sensitivity, "fsdp", axis=0, tiled=True),
        (((0,), (0,)), ((), ())),
        preferred_element_type=jnp.float32,
    )
    weight_grad = lax.psum_scatter(decode_sum * group_block, "grp", scatter_dimension=0, tiled=True)
    return (input_grad, weight_grad)


def encode(value):
    top = jnp.maximum(jnp.max(jnp.abs(value), axis=0, keepdims=True), TINY)
    coded = jnp.round(value * (STEPS / top)).astype(jnp.int32).astype(jnp.int16)
    return coded, top * (1.0 / STEPS)


def decoded(coded, step):
    return coded.astype(jnp.int32).astype(jnp.float32) * step


def kernel(
    deep,
    mask_hbm, list_hbm, x_hbm, s_hbm, w_hbm,
    ig_ref, wg_ref,
    mask_ref, list_ref,
    x_v, s_v, w_v, tx, rx, own_part, px_send, px_scale, px_recv, px_rscale,
    q, q_send, q_scale, zr, zr_scale, ig_send,
    load_sem, s_send_sem, s_recv_sem, x_send_sem, x_recv_sem,
    px_send_sem, px_recv_sem, z_send_sem, z_recv_sem, ig_send_sem, ig_recv_sem, hello,
):
    grp = lax.axis_index("grp")
    y = lax.axis_index("fsdp")
    core = lax.rem(grp, CORES)
    wide = lax.rem(grp // CORES, WIDE)
    z = grp // (CORES * WIDE)
    oy, oc = 1 - y, 1 - core
    tokens = s_hbm.shape[0]
    groups = mask_ref.shape[0]
    rows = wg_ref.shape[0]
    half = w_hbm.shape[0]
    part_tokens = tokens // 2
    part_rows = rows // HALVES
    pieces = deep * HALVES

    def at(zz, xx, cc, yy):
        return ((zz * WIDE + xx) * CORES + cc, yy)

    def remote(src, dst, send, recv, device):
        return pltpu.make_async_remote_copy(
            src_ref=src, dst_ref=dst, send_sem=send, recv_sem=recv,
            device_id=device, device_id_type=MESH,
        )

    y_peer = at(z, wide, core, oy)
    y_cross = at(z, wide, oc, oy)
    sibling = at(z, wide, oc, y)
    x_peer = at(z, 1 - wide, core, y)
    below = at(lax.rem(z + deep - 1, deep), wide, core, y)
    above = at(lax.rem(z + 1, deep), wide, core, y)
    me = core * 2 + y
    from_y = core * 2 + oy
    from_cross = oc * 2 + oy
    from_sib = oc * 2 + y

    barrier = pltpu.get_barrier_semaphore()
    partners = [y_peer, y_cross, sibling, x_peer]
    for partner in partners:
        pl.semaphore_signal(barrier, inc=1, device_id=partner, device_id_type=MESH)

    @pl.when(z > 0)
    def _():
        pl.semaphore_signal(barrier, inc=1, device_id=below, device_id_type=MESH)

    @pl.when(z < deep - 1)
    def _():
        pl.semaphore_signal(barrier, inc=1, device_id=above, device_id_type=MESH)

    load_x = pltpu.make_async_copy(x_hbm, x_v, load_sem.at[0])
    load_s = pltpu.make_async_copy(s_hbm, s_v.at[me], load_sem.at[1])
    load_w = pltpu.make_async_copy(w_hbm, w_v, load_sem.at[2])
    load_mask = pltpu.make_async_copy(mask_hbm, mask_ref, load_sem.at[3])
    load_list = pltpu.make_async_copy(list_hbm, list_ref, load_sem.at[4])
    loads = [load_x, load_s, load_w, load_mask, load_list]
    for load in loads:
        load.start()

    first, second = pl.ds(0, part_tokens), pl.ds(part_tokens, part_tokens)
    def received(ref, sem):
        remote(ref, ref, sem, sem, sibling).wait_recv()

    def sent(ref, sem):
        remote(ref, ref, sem, sem, sibling).wait_send()

    s_y = remote(s_hbm.at[first], s_v.at[me, first], s_send_sem, s_recv_sem.at[0], y_peer)
    s_cross = remote(s_hbm.at[second], s_v.at[me, second], s_send_sem, s_recv_sem.at[0], y_cross)
    s_sib = remote(s_hbm, s_v.at[me], s_send_sem, s_recv_sem.at[1], sibling)
    forward_y = remote(s_v.at[from_y, first], s_v.at[from_y, first], s_send_sem, s_recv_sem.at[1], sibling)
    forward_cross = remote(
        s_v.at[from_cross, second], s_v.at[from_cross, second], s_send_sem, s_recv_sem.at[1], sibling
    )

    @pl.when(jnp.logical_and(z > 0, z < deep - 1))
    def _():
        pl.semaphore_wait(barrier, len(partners) + 2)

    @pl.when(jnp.logical_or(z == 0, z == deep - 1))
    def _():
        pl.semaphore_wait(barrier, len(partners) + 1)

    s_y.start()
    s_cross.start()
    s_sib.start()

    @pl.when(z == deep - 2)
    def _():
        pl.semaphore_signal(hello.at[0], inc=1, device_id=below, device_id_type=MESH)

    @pl.when(z == 1)
    def _():
        pl.semaphore_signal(hello.at[1], inc=1, device_id=above, device_id_type=MESH)

    span = WIDE * CORES * 2 * rows

    def plane(n):
        if n == deep - 1:
            return z
        down = jnp.where(deep - 1 - n > z, deep - 1 - n, deep - 2 - n)
        return jnp.where(z < deep // 2, down, jnp.where(n < z, n, n + 1))

    def turn(n):
        part = x_v[:, pl.ds(pl.multiple_of(plane(n) * span, span), span)].T
        for xx in range(WIDE):
            for cy in range(CORES * 2):
                for h in range(HALVES):
                    start = (xx * CORES * 2 + cy) * rows + h * part_rows
                    tx[n * HALVES + h, cy, xx * part_rows:(xx + 1) * part_rows, :] = part[start:start + part_rows, :]

    load_x.wait()
    for n in range(deep):
        turn(n)
        for j in range(n * HALVES, (n + 1) * HALVES):
            for device, there in ((y_peer, from_y), (y_cross, from_cross), (sibling, from_sib)):
                remote(tx.at[j, there], rx.at[j, me], x_send_sem, x_recv_sem.at[j], device).start()
            rx[j, me] = tx[j, me]

    load_mask.wait()
    load_list.wait()
    scales = []
    for cc in range(CORES):
        here = (z * WIDE + wide) * CORES + cc
        mine = list_ref[here]
        tally = jnp.int32(0)
        for h in range(groups):
            tally = tally + jnp.where(list_ref[h] == mine, mask_ref[h], 0)
        done = jnp.full((1, wg_ref.shape[1]), mask_ref[here], jnp.int32).astype(jnp.float32)
        total = jnp.full((1, wg_ref.shape[1]), tally, jnp.int32).astype(jnp.float32)
        scales.append(done / (total + 1.0 - done))

    load_s.wait()
    load_w.wait()

    def grad(s_block):
        return lax.dot_general(
            s_block, w_v[...], (((1,), (1,)), ((), ())), preferred_element_type=jnp.float32
        ).astype(jnp.bfloat16)

    own_columns = pl.ds(pl.multiple_of(y * half, half), half)
    ig_ref[:, own_columns] = grad(s_v[me])

    received(s_v.at[me], s_recv_sem.at[0])
    forward_y.start()
    forward_cross.start()
    ig_send[...] = grad(jnp.concatenate([s_v[from_y, first], s_v[from_cross, second]], axis=0))
    remote(ig_send.at[first], ig_ref.at[first, own_columns], ig_send_sem, ig_recv_sem, y_peer).start()
    remote(ig_send.at[second], ig_ref.at[second, own_columns], ig_send_sem, ig_recv_sem, y_cross).start()

    @pl.when(jnp.logical_and(z > 0, z < deep - 2))
    def _():
        pl.semaphore_wait(hello.at[0], 1)
        pl.semaphore_signal(hello.at[0], inc=1, device_id=below, device_id_type=MESH)

    @pl.when(jnp.logical_and(z > 1, z < deep - 1))
    def _():
        pl.semaphore_wait(hello.at[1], 1)
        pl.semaphore_signal(hello.at[1], inc=1, device_id=above, device_id_type=MESH)

    received(s_v.at[0:2], s_recv_sem.at[1])

    def partial(j):
        received(rx.at[j, 0:3], x_recv_sem.at[j])
        total = None
        for cc in range(CORES):
            left = jnp.concatenate([rx[j, cc * 2], rx[j, cc * 2 + 1]], axis=1)
            right = s_v[cc * 2:cc * 2 + 2].reshape(2 * tokens, s_v.shape[2])
            product = scales[cc] * jnp.dot(left, right, preferred_element_type=jnp.float32)
            total = product if total is None else total + product
        own_part[j, 0] = total[:part_rows]
        own_part[j, 1] = total[part_rows:]
        coded, scale = encode(own_part[j, 1 - wide])
        px_send[j] = coded
        px_scale[j] = scale
        remote(px_send.at[j], px_recv.at[j], px_send_sem.at[0], px_recv_sem.at[j, 0], x_peer).start()
        remote(px_scale.at[j], px_rscale.at[j], px_send_sem.at[1], px_recv_sem.at[j, 1], x_peer).start()

    def gather_x(j):
        n, h = j // HALVES, j % HALVES
        if j == 0:
            @pl.when(z == 0)
            def _():
                pl.semaphore_wait(hello.at[0], 1)

            @pl.when(z == deep - 1)
            def _():
                pl.semaphore_wait(hello.at[1], 1)

        received(px_recv.at[j], px_recv_sem.at[j, 0])
        received(px_rscale.at[j], px_recv_sem.at[j, 1])
        value = own_part[j, wide] + decoded(px_recv[j], px_rscale[j])
        if n < deep - 1:
            coded, scale = encode(value)
            q_send[j] = coded
            q_scale[j] = scale
            there = at(plane(n), wide, core, y)
            remote(q_send.at[j], zr.at[z, h], z_send_sem.at[0], z_recv_sem.at[z, 0], there).start()
            remote(q_scale.at[j], zr_scale.at[z, h], z_send_sem.at[1], z_recv_sem.at[z, 1], there).start()
        else:
            q[h] = value

    for j in range(pieces + LAG):
        if j < pieces:
            partial(j)
        if j >= LAG:
            gather_x(j - LAG)

    sent(s_v.at[0:3], s_send_sem)
    sent(tx.at[:, 0:3], x_send_sem)
    sent(px_send, px_send_sem.at[0])
    sent(px_scale, px_send_sem.at[1])
    sent(q_send, z_send_sem.at[0])
    sent(q_scale, z_send_sem.at[1])
    sent(ig_send, ig_send_sem)

    for n in range(deep - 1):
        source = jnp.where(n < z, n, n + 1)
        received(zr.at[source], z_recv_sem.at[source, 0])
        received(zr_scale.at[source], z_recv_sem.at[source, 1])
        for h in range(HALVES):
            value = decoded(zr[source, h], zr_scale[source, h])
            if n < deep - 2:
                q[h] = q[h] + value
            else:
                wg_ref[h * part_rows:(h + 1) * part_rows, :] = q[h] + value

    received(ig_send, ig_recv_sem)


def write_out(ig_ref, wg_ref, ig_hbm, wg_hbm, sems):
    copies = [
        pltpu.make_async_copy(ig_ref, ig_hbm, sems.at[0]),
        pltpu.make_async_copy(wg_ref, wg_hbm, sems.at[1]),
    ]
    for copy in copies:
        copy.start()
    for copy in copies:
        copy.wait()


def kernel_shards(deep, rows, x, s, w, mask, plist):
    tokens, width = x.shape
    values = s.shape[1]
    f32, bf16, i16 = jnp.float32, jnp.bfloat16, jnp.int16
    dma = pltpu.SemaphoreType.DMA
    anywhere = pl.BlockSpec(memory_space=pl.ANY)
    part_rows, pieces = rows // HALVES, deep * HALVES
    on_chip = pl.pallas_call(
        functools.partial(kernel, deep),
        out_shape=(
            pltpu.VMEM((tokens, width), bf16),
            pltpu.VMEM((rows, values), f32),
        ),
        in_specs=[anywhere] * 5,
        out_specs=(pl.BlockSpec(memory_space=pltpu.VMEM),) * 2,
        scratch_shapes=[
            pltpu.SMEM(mask.shape, jnp.int32),
            pltpu.SMEM(plist.shape, jnp.int32),
            pltpu.VMEM((tokens, width), bf16),
            pltpu.VMEM((CORES * 2, tokens, values), bf16),
            pltpu.VMEM(w.shape, bf16),
            pltpu.VMEM((pieces, CORES * 2, WIDE * part_rows, tokens), bf16),
            pltpu.VMEM((pieces, CORES * 2, WIDE * part_rows, tokens), bf16),
            pltpu.VMEM((pieces, WIDE, part_rows, values), f32),
            pltpu.VMEM((pieces, part_rows, values), i16),
            pltpu.VMEM((pieces, 1, values), f32),
            pltpu.VMEM((pieces, part_rows, values), i16),
            pltpu.VMEM((pieces, 1, values), f32),
            pltpu.VMEM((HALVES, part_rows, values), f32),
            pltpu.VMEM((pieces - HALVES, part_rows, values), i16),
            pltpu.VMEM((pieces - HALVES, 1, values), f32),
            pltpu.VMEM((deep, HALVES, part_rows, values), i16),
            pltpu.VMEM((deep, HALVES, 1, values), f32),
            pltpu.VMEM((tokens, w.shape[0]), bf16),
            dma((5,)), dma, dma((2,)), dma, dma((pieces,)),
            dma((2,)), dma((pieces, 2)), dma((2,)), dma((deep, 2)), dma, dma,
            pltpu.SemaphoreType.REGULAR((2,)),
        ],
        compiler_params=pltpu.CompilerParams(collective_id=0, has_side_effects=True),
    )(mask, plist, x, s, w)
    return pl.pallas_call(
        write_out,
        out_shape=(
            jax.ShapeDtypeStruct((tokens, width), bf16),
            jax.ShapeDtypeStruct((rows, values), f32),
        ),
        in_specs=[pl.BlockSpec(memory_space=pltpu.VMEM)] * 2,
        out_specs=(anywhere,) * 2,
        scratch_shapes=[dma((2,))],
        compiler_params=pltpu.CompilerParams(vmem_limit_bytes=SMALL),
    )(*(pltpu.with_memory_space_constraint(part, pltpu.VMEM) for part in on_chip))


def solution(mesh):
    outer, inner = mesh.shape["grp"], mesh.shape["fsdp"]

    def shards(x, s, w, mask, plist):
        rows = x.shape[1] // (outer * inner)
        if inner == 2 and outer % (CORES * WIDE) == 0 and outer // (CORES * WIDE) >= 4 and rows % (16 * HALVES) == 0 and x.shape[0] % 128 == 0:
            return tuple(kernel_shards(outer // (CORES * WIDE), rows, x, s, w, mask, plist))
        return collective_shards(x, s, w, mask, plist)

    in_specs = (P(("grp", "fsdp"), None), P(("grp", "fsdp"), None), P("fsdp", None), P(), P())
    out_specs = (P(("grp", "fsdp"), None), P(("grp", "fsdp"), None))
    return jax.shard_map(shards, mesh=mesh, in_specs=in_specs, out_specs=out_specs, check_vma=False)
```

```python
import functools

import jax
import jax.numpy as jnp
from jax import lax
from jax.experimental import pallas as pl
from jax.experimental.pallas import tpu as pltpu
from jax.sharding import PartitionSpec as P

MESH = pl.DeviceIdType.MESH
CORES = 2
WIDE = 2
HALVES = 2
LAG = 4
ORDERS = {4: ((3, 1, 2), (0, 3, 2), (0, 3, 1), (0, 2, 1))}
SMALL = 1 << 20
STEPS = 32766.0
TINY = 1e-33


def collective_shards(
    normalized_inputs,
    output_sensitivity,
    projection_weights,
    completion_mask,
    replica_partition_list,
):
    replica_index = lax.axis_index("grp")
    selected_replica = lax.iota(jnp.int32, completion_mask.shape[0]) == replica_index
    assigned_piece = jnp.sum(jnp.where(selected_replica, replica_partition_list, 0))
    finished_indicator = jnp.sum(jnp.where(selected_replica, completion_mask, 0))
    finisher_tally = jnp.sum(
        jnp.where(replica_partition_list == assigned_piece, completion_mask, 0)
    )
    living_float = finished_indicator.astype(jnp.float32)
    decode_sum = living_float / (finisher_tally.astype(jnp.float32) + 1.0 - living_float)
    tokens_here = normalized_inputs.shape[0]
    model_width = normalized_inputs.shape[1]
    inner_size = lax.axis_size("fsdp")
    outer_size = lax.axis_size("grp")
    input_grad = lax.dot_general(
        output_sensitivity,
        lax.all_gather(projection_weights, "fsdp", axis=0, tiled=True),
        (((1,), (1,)), ((), ())),
        preferred_element_type=jnp.float32,
    ).astype(jnp.bfloat16)
    owner_rows = model_width // (outer_size * inner_size)
    reordered = normalized_inputs.reshape(tokens_here, outer_size, inner_size, owner_rows)
    reordered = reordered.transpose(0, 2, 1, 3).reshape(tokens_here, model_width)
    column_block = lax.all_to_all(reordered, "fsdp", split_axis=1, concat_axis=0, tiled=True)
    group_block = lax.dot_general(
        column_block,
        lax.all_gather(output_sensitivity, "fsdp", axis=0, tiled=True),
        (((0,), (0,)), ((), ())),
        preferred_element_type=jnp.float32,
    )
    weight_grad = lax.psum_scatter(decode_sum * group_block, "grp", scatter_dimension=0, tiled=True)
    return (input_grad, weight_grad)


def encode(value):
    top = jnp.maximum(jnp.max(jnp.abs(value), axis=0, keepdims=True), TINY)
    coded = jnp.round(value * (STEPS / top)).astype(jnp.int32).astype(jnp.int16)
    return coded, top * (1.0 / STEPS)


def decoded(coded, step):
    return coded.astype(jnp.int32).astype(jnp.float32) * step


def kernel(
    deep,
    mask_hbm, list_hbm, x_hbm, s_hbm, w_hbm,
    ig_ref, wg_ref,
    mask_ref, list_ref,
    x_v, s_v, w_v, tx, rx, own_part, px_send, px_scale, px_recv, px_rscale,
    q, q_send, q_scale, zr, zr_scale, ig_send,
    load_sem, s_send_sem, s_recv_sem, x_send_sem, x_recv_sem,
    px_send_sem, px_recv_sem, z_send_sem, z_recv_sem, ig_send_sem, ig_recv_sem, hello,
):
    grp = lax.axis_index("grp")
    y = lax.axis_index("fsdp")
    core = lax.rem(grp, CORES)
    wide = lax.rem(grp // CORES, WIDE)
    z = grp // (CORES * WIDE)
    oy, oc = 1 - y, 1 - core
    tokens = s_hbm.shape[0]
    groups = mask_ref.shape[0]
    rows = wg_ref.shape[0]
    half = w_hbm.shape[0]
    part_tokens = tokens // 2
    part_rows = rows // HALVES
    pieces = deep * HALVES

    def at(zz, xx, cc, yy):
        return ((zz * WIDE + xx) * CORES + cc, yy)

    def remote(src, dst, send, recv, device):
        return pltpu.make_async_remote_copy(
            src_ref=src, dst_ref=dst, send_sem=send, recv_sem=recv,
            device_id=device, device_id_type=MESH,
        )

    y_peer = at(z, wide, core, oy)
    y_cross = at(z, wide, oc, oy)
    sibling = at(z, wide, oc, y)
    x_peer = at(z, 1 - wide, core, y)
    below = at(lax.rem(z + deep - 1, deep), wide, core, y)
    above = at(lax.rem(z + 1, deep), wide, core, y)
    me = core * 2 + y
    from_y = core * 2 + oy
    from_cross = oc * 2 + oy
    from_sib = oc * 2 + y

    barrier = pltpu.get_barrier_semaphore()
    partners = [y_peer, y_cross, sibling, x_peer]
    for partner in partners:
        pl.semaphore_signal(barrier, inc=1, device_id=partner, device_id_type=MESH)

    @pl.when(z > 0)
    def _():
        pl.semaphore_signal(barrier, inc=1, device_id=below, device_id_type=MESH)

    @pl.when(z < deep - 1)
    def _():
        pl.semaphore_signal(barrier, inc=1, device_id=above, device_id_type=MESH)

    load_x = pltpu.make_async_copy(x_hbm, x_v, load_sem.at[0])
    load_s = pltpu.make_async_copy(s_hbm, s_v.at[me], load_sem.at[1])
    load_w = pltpu.make_async_copy(w_hbm, w_v, load_sem.at[2])
    load_mask = pltpu.make_async_copy(mask_hbm, mask_ref, load_sem.at[3])
    load_list = pltpu.make_async_copy(list_hbm, list_ref, load_sem.at[4])
    loads = [load_x, load_s, load_w, load_mask, load_list]
    for load in loads:
        load.start()

    first, second = pl.ds(0, part_tokens), pl.ds(part_tokens, part_tokens)
    def received(ref, sem):
        remote(ref, ref, sem, sem, sibling).wait_recv()

    def sent(ref, sem):
        remote(ref, ref, sem, sem, sibling).wait_send()

    s_y = remote(s_hbm.at[first], s_v.at[me, first], s_send_sem, s_recv_sem.at[0], y_peer)
    s_cross = remote(s_hbm.at[second], s_v.at[me, second], s_send_sem, s_recv_sem.at[0], y_cross)
    s_sib = remote(s_hbm, s_v.at[me], s_send_sem, s_recv_sem.at[1], sibling)
    forward_y = remote(s_v.at[from_y, first], s_v.at[from_y, first], s_send_sem, s_recv_sem.at[1], sibling)
    forward_cross = remote(
        s_v.at[from_cross, second], s_v.at[from_cross, second], s_send_sem, s_recv_sem.at[1], sibling
    )

    @pl.when(jnp.logical_and(z > 0, z < deep - 1))
    def _():
        pl.semaphore_wait(barrier, len(partners) + 2)

    @pl.when(jnp.logical_or(z == 0, z == deep - 1))
    def _():
        pl.semaphore_wait(barrier, len(partners) + 1)

    s_y.start()
    s_cross.start()
    s_sib.start()

    @pl.when(z == deep - 2)
    def _():
        pl.semaphore_signal(hello.at[0], inc=1, device_id=below, device_id_type=MESH)

    @pl.when(z == 1)
    def _():
        pl.semaphore_signal(hello.at[1], inc=1, device_id=above, device_id_type=MESH)

    span = WIDE * CORES * 2 * rows

    orders = ORDERS.get(deep) or [[p for p in range(deep) if p != own] for own in range(deep)]

    def plane(n):
        if n == deep - 1:
            return z
        there = jnp.int32(0)
        for own in range(deep):
            there = jnp.where(z == own, orders[own][n], there)
        return there

    def turn(n):
        part = x_v[:, pl.ds(pl.multiple_of(plane(n) * span, span), span)].T
        for xx in range(WIDE):
            for cy in range(CORES * 2):
                for h in range(HALVES):
                    start = (xx * CORES * 2 + cy) * rows + h * part_rows
                    tx[n * HALVES + h, cy, xx * part_rows:(xx + 1) * part_rows, :] = part[start:start + part_rows, :]

    load_x.wait()
    for n in range(deep):
        turn(n)
        for j in range(n * HALVES, (n + 1) * HALVES):
            for device, there in ((y_peer, from_y), (y_cross, from_cross), (sibling, from_sib)):
                remote(tx.at[j, there], rx.at[j, me], x_send_sem, x_recv_sem.at[j], device).start()
            rx[j, me] = tx[j, me]

    load_mask.wait()
    load_list.wait()
    scales = []
    for cc in range(CORES):
        here = (z * WIDE + wide) * CORES + cc
        mine = list_ref[here]
        tally = jnp.int32(0)
        for h in range(groups):
            tally = tally + jnp.where(list_ref[h] == mine, mask_ref[h], 0)
        done = jnp.full((1, wg_ref.shape[1]), mask_ref[here], jnp.int32).astype(jnp.float32)
        total = jnp.full((1, wg_ref.shape[1]), tally, jnp.int32).astype(jnp.float32)
        scales.append(done / (total + 1.0 - done))

    load_s.wait()
    load_w.wait()

    def grad(s_block):
        return lax.dot_general(
            s_block, w_v[...], (((1,), (1,)), ((), ())), preferred_element_type=jnp.float32
        ).astype(jnp.bfloat16)

    own_columns = pl.ds(pl.multiple_of(y * half, half), half)
    ig_ref[:, own_columns] = grad(s_v[me])

    received(s_v.at[me], s_recv_sem.at[0])
    forward_y.start()
    forward_cross.start()
    ig_send[...] = grad(jnp.concatenate([s_v[from_y, first], s_v[from_cross, second]], axis=0))
    remote(ig_send.at[first], ig_ref.at[first, own_columns], ig_send_sem, ig_recv_sem, y_peer).start()
    remote(ig_send.at[second], ig_ref.at[second, own_columns], ig_send_sem, ig_recv_sem, y_cross).start()

    @pl.when(jnp.logical_and(z > 0, z < deep - 2))
    def _():
        pl.semaphore_wait(hello.at[0], 1)
        pl.semaphore_signal(hello.at[0], inc=1, device_id=below, device_id_type=MESH)

    @pl.when(jnp.logical_and(z > 1, z < deep - 1))
    def _():
        pl.semaphore_wait(hello.at[1], 1)
        pl.semaphore_signal(hello.at[1], inc=1, device_id=above, device_id_type=MESH)

    received(s_v.at[0:2], s_recv_sem.at[1])

    def partial(j):
        received(rx.at[j, 0:3], x_recv_sem.at[j])
        total = None
        for cc in range(CORES):
            left = jnp.concatenate([rx[j, cc * 2], rx[j, cc * 2 + 1]], axis=1)
            right = s_v[cc * 2:cc * 2 + 2].reshape(2 * tokens, s_v.shape[2])
            product = scales[cc] * jnp.dot(left, right, preferred_element_type=jnp.float32)
            total = product if total is None else total + product
        own_part[j, 0] = total[:part_rows]
        own_part[j, 1] = total[part_rows:]
        coded, scale = encode(own_part[j, 1 - wide])
        px_send[j] = coded
        px_scale[j] = scale
        remote(px_send.at[j], px_recv.at[j], px_send_sem.at[0], px_recv_sem.at[j, 0], x_peer).start()
        remote(px_scale.at[j], px_rscale.at[j], px_send_sem.at[1], px_recv_sem.at[j, 1], x_peer).start()

    def gather_x(j):
        n, h = j // HALVES, j % HALVES
        if j == 0:
            @pl.when(z == 0)
            def _():
                pl.semaphore_wait(hello.at[0], 1)

            @pl.when(z == deep - 1)
            def _():
                pl.semaphore_wait(hello.at[1], 1)

        received(px_recv.at[j], px_recv_sem.at[j, 0])
        received(px_rscale.at[j], px_recv_sem.at[j, 1])
        value = own_part[j, wide] + decoded(px_recv[j], px_rscale[j])
        if n < deep - 1:
            coded, scale = encode(value)
            q_send[j] = coded
            q_scale[j] = scale
            there = at(plane(n), wide, core, y)
            remote(q_send.at[j], zr.at[z, h], z_send_sem.at[0], z_recv_sem.at[z, 0], there).start()
            remote(q_scale.at[j], zr_scale.at[z, h], z_send_sem.at[1], z_recv_sem.at[z, 1], there).start()
        else:
            q[h] = value

    for j in range(pieces + LAG):
        if j < pieces:
            partial(j)
        if j >= LAG:
            gather_x(j - LAG)

    sent(s_v.at[0:3], s_send_sem)
    sent(tx.at[:, 0:3], x_send_sem)
    sent(px_send, px_send_sem.at[0])
    sent(px_scale, px_send_sem.at[1])
    sent(q_send, z_send_sem.at[0])
    sent(q_scale, z_send_sem.at[1])
    sent(ig_send, ig_send_sem)

    for n in range(deep - 1):
        source = jnp.where(n < z, n, n + 1)
        received(zr.at[source], z_recv_sem.at[source, 0])
        received(zr_scale.at[source], z_recv_sem.at[source, 1])
        for h in range(HALVES):
            value = decoded(zr[source, h], zr_scale[source, h])
            if n < deep - 2:
                q[h] = q[h] + value
            else:
                wg_ref[h * part_rows:(h + 1) * part_rows, :] = q[h] + value

    received(ig_send, ig_recv_sem)


def write_out(ig_ref, wg_ref, ig_hbm, wg_hbm, sems):
    copies = [
        pltpu.make_async_copy(ig_ref, ig_hbm, sems.at[0]),
        pltpu.make_async_copy(wg_ref, wg_hbm, sems.at[1]),
    ]
    for copy in copies:
        copy.start()
    for copy in copies:
        copy.wait()


def kernel_shards(deep, rows, x, s, w, mask, plist):
    tokens, width = x.shape
    values = s.shape[1]
    f32, bf16, i16 = jnp.float32, jnp.bfloat16, jnp.int16
    dma = pltpu.SemaphoreType.DMA
    anywhere = pl.BlockSpec(memory_space=pl.ANY)
    part_rows, pieces = rows // HALVES, deep * HALVES
    on_chip = pl.pallas_call(
        functools.partial(kernel, deep),
        out_shape=(
            pltpu.VMEM((tokens, width), bf16),
            pltpu.VMEM((rows, values), f32),
        ),
        in_specs=[anywhere] * 5,
        out_specs=(pl.BlockSpec(memory_space=pltpu.VMEM),) * 2,
        scratch_shapes=[
            pltpu.SMEM(mask.shape, jnp.int32),
            pltpu.SMEM(plist.shape, jnp.int32),
            pltpu.VMEM((tokens, width), bf16),
            pltpu.VMEM((CORES * 2, tokens, values), bf16),
            pltpu.VMEM(w.shape, bf16),
            pltpu.VMEM((pieces, CORES * 2, WIDE * part_rows, tokens), bf16),
            pltpu.VMEM((pieces, CORES * 2, WIDE * part_rows, tokens), bf16),
            pltpu.VMEM((pieces, WIDE, part_rows, values), f32),
            pltpu.VMEM((pieces, part_rows, values), i16),
            pltpu.VMEM((pieces, 1, values), f32),
            pltpu.VMEM((pieces, part_rows, values), i16),
            pltpu.VMEM((pieces, 1, values), f32),
            pltpu.VMEM((HALVES, part_rows, values), f32),
            pltpu.VMEM((pieces - HALVES, part_rows, values), i16),
            pltpu.VMEM((pieces - HALVES, 1, values), f32),
            pltpu.VMEM((deep, HALVES, part_rows, values), i16),
            pltpu.VMEM((deep, HALVES, 1, values), f32),
            pltpu.VMEM((tokens, w.shape[0]), bf16),
            dma((5,)), dma, dma((2,)), dma, dma((pieces,)),
            dma((2,)), dma((pieces, 2)), dma((2,)), dma((deep, 2)), dma, dma,
            pltpu.SemaphoreType.REGULAR((2,)),
        ],
        compiler_params=pltpu.CompilerParams(collective_id=0, has_side_effects=True),
    )(mask, plist, x, s, w)
    return pl.pallas_call(
        write_out,
        out_shape=(
            jax.ShapeDtypeStruct((tokens, width), bf16),
            jax.ShapeDtypeStruct((rows, values), f32),
        ),
        in_specs=[pl.BlockSpec(memory_space=pltpu.VMEM)] * 2,
        out_specs=(anywhere,) * 2,
        scratch_shapes=[dma((2,))],
        compiler_params=pltpu.CompilerParams(vmem_limit_bytes=SMALL),
    )(*(pltpu.with_memory_space_constraint(part, pltpu.VMEM) for part in on_chip))


def solution(mesh):
    outer, inner = mesh.shape["grp"], mesh.shape["fsdp"]

    def shards(x, s, w, mask, plist):
        rows = x.shape[1] // (outer * inner)
        if inner == 2 and outer % (CORES * WIDE) == 0 and outer // (CORES * WIDE) >= 4 and rows % (16 * HALVES) == 0 and x.shape[0] % 128 == 0:
            return tuple(kernel_shards(outer // (CORES * WIDE), rows, x, s, w, mask, plist))
        return collective_shards(x, s, w, mask, plist)

    in_specs = (P(("grp", "fsdp"), None), P(("grp", "fsdp"), None), P("fsdp", None), P(), P())
    out_specs = (P(("grp", "fsdp"), None), P(("grp", "fsdp"), None))
    return jax.shard_map(shards, mesh=mesh, in_specs=in_specs, out_specs=out_specs, check_vma=False)
```

```python
import functools

import jax
import jax.numpy as jnp
from jax import lax
from jax.experimental import pallas as pl
from jax.experimental.pallas import tpu as pltpu
from jax.sharding import PartitionSpec as P

MESH = pl.DeviceIdType.MESH
CORES = 2
WIDE = 2
HALVES = 2
STRIPS = 4
LAG = 1
ORDERS = {4: ((3, 2, 1), (0, 3, 2), (0, 3, 1), (0, 1, 2))}
SMALL = 1 << 20
STEPS = 32766.0
TINY = 1e-33


def collective_shards(
    normalized_inputs,
    output_sensitivity,
    projection_weights,
    completion_mask,
    replica_partition_list,
):
    replica_index = lax.axis_index("grp")
    selected_replica = lax.iota(jnp.int32, completion_mask.shape[0]) == replica_index
    assigned_piece = jnp.sum(jnp.where(selected_replica, replica_partition_list, 0))
    finished_indicator = jnp.sum(jnp.where(selected_replica, completion_mask, 0))
    finisher_tally = jnp.sum(
        jnp.where(replica_partition_list == assigned_piece, completion_mask, 0)
    )
    living_float = finished_indicator.astype(jnp.float32)
    decode_sum = living_float / (finisher_tally.astype(jnp.float32) + 1.0 - living_float)
    tokens_here = normalized_inputs.shape[0]
    model_width = normalized_inputs.shape[1]
    inner_size = lax.axis_size("fsdp")
    outer_size = lax.axis_size("grp")
    input_grad = lax.dot_general(
        output_sensitivity,
        lax.all_gather(projection_weights, "fsdp", axis=0, tiled=True),
        (((1,), (1,)), ((), ())),
        preferred_element_type=jnp.float32,
    ).astype(jnp.bfloat16)
    owner_rows = model_width // (outer_size * inner_size)
    reordered = normalized_inputs.reshape(tokens_here, outer_size, inner_size, owner_rows)
    reordered = reordered.transpose(0, 2, 1, 3).reshape(tokens_here, model_width)
    column_block = lax.all_to_all(reordered, "fsdp", split_axis=1, concat_axis=0, tiled=True)
    group_block = lax.dot_general(
        column_block,
        lax.all_gather(output_sensitivity, "fsdp", axis=0, tiled=True),
        (((0,), (0,)), ((), ())),
        preferred_element_type=jnp.float32,
    )
    weight_grad = lax.psum_scatter(decode_sum * group_block, "grp", scatter_dimension=0, tiled=True)
    return (input_grad, weight_grad)


def encode(value):
    top = jnp.maximum(jnp.max(jnp.abs(value), axis=0, keepdims=True), TINY)
    coded = jnp.round(value * (STEPS / top)).astype(jnp.int32).astype(jnp.int16)
    return coded, top * (1.0 / STEPS)


def decoded(coded, step):
    return coded.astype(jnp.int32).astype(jnp.float32) * step


def kernel(
    deep,
    mask_hbm, list_hbm, x_hbm, s_hbm, w_hbm,
    ig_ref, wg_ref,
    mask_ref, list_ref,
    x_v, s_v, w_v, lead_tx, lead_rx, tx, rx,
    lead_part, lead_send, lead_scale, lead_recv, lead_rscale, lead_q, lead_qscale,
    own_part, px_send, px_scale, px_recv, px_rscale, q, q_send, q_scale, zr, zr_scale, ig_send,
    load_sem, s_send_sem, s_recv_sem, x_send_sem, x_recv_sem,
    px_send_sem, lead_recv_sem, px_recv_sem, z_send_sem, z_recv_sem, ig_send_sem, ig_recv_sem, hello,
):
    grp = lax.axis_index("grp")
    y = lax.axis_index("fsdp")
    core = lax.rem(grp, CORES)
    wide = lax.rem(grp // CORES, WIDE)
    z = grp // (CORES * WIDE)
    oy, oc = 1 - y, 1 - core
    tokens = s_hbm.shape[0]
    groups = mask_ref.shape[0]
    rows = wg_ref.shape[0]
    half = w_hbm.shape[0]
    part_tokens = tokens // 2
    part_rows = rows // HALVES
    pieces = (deep - 1) * HALVES
    strip = s_hbm.shape[1] // STRIPS

    def at(zz, xx, cc, yy):
        return ((zz * WIDE + xx) * CORES + cc, yy)

    def remote(src, dst, send, recv, device):
        return pltpu.make_async_remote_copy(
            src_ref=src, dst_ref=dst, send_sem=send, recv_sem=recv,
            device_id=device, device_id_type=MESH,
        )

    y_peer = at(z, wide, core, oy)
    y_cross = at(z, wide, oc, oy)
    sibling = at(z, wide, oc, y)
    x_peer = at(z, 1 - wide, core, y)
    below = at(lax.rem(z + deep - 1, deep), wide, core, y)
    above = at(lax.rem(z + 1, deep), wide, core, y)
    me = core * 2 + y
    from_y = core * 2 + oy
    from_cross = oc * 2 + oy
    from_sib = oc * 2 + y

    barrier = pltpu.get_barrier_semaphore()
    partners = [y_peer, y_cross, sibling, x_peer]
    for partner in partners:
        pl.semaphore_signal(barrier, inc=1, device_id=partner, device_id_type=MESH)

    @pl.when(z > 0)
    def _():
        pl.semaphore_signal(barrier, inc=1, device_id=below, device_id_type=MESH)

    @pl.when(z < deep - 1)
    def _():
        pl.semaphore_signal(barrier, inc=1, device_id=above, device_id_type=MESH)

    load_x = pltpu.make_async_copy(x_hbm, x_v, load_sem.at[0])
    load_w = pltpu.make_async_copy(w_hbm, w_v, load_sem.at[2])
    load_mask = pltpu.make_async_copy(mask_hbm, mask_ref, load_sem.at[3])
    load_list = pltpu.make_async_copy(list_hbm, list_ref, load_sem.at[4])
    columns = [pl.ds(k * strip, strip) for k in range(STRIPS)]
    load_x.start()
    for k in range(STRIPS):
        pltpu.make_async_copy(s_hbm.at[:, columns[k]], s_v.at[k, me], load_sem.at[1]).start()
    load_w.start()
    load_mask.start()
    load_list.start()

    first, second = pl.ds(0, part_tokens), pl.ds(part_tokens, part_tokens)
    def received(ref, sem):
        remote(ref, ref, sem, sem, sibling).wait_recv()

    def sent(ref, sem):
        remote(ref, ref, sem, sem, sibling).wait_send()

    def send_strip(k):
        own = s_v.at[k, me]
        remote(s_hbm.at[first, columns[k]], own.at[first], s_send_sem, s_recv_sem.at[k, 0], y_peer).start()
        remote(s_hbm.at[second, columns[k]], own.at[second], s_send_sem, s_recv_sem.at[k, 0], y_cross).start()
        remote(s_hbm.at[:, columns[k]], own, s_send_sem, s_recv_sem.at[k, 1], sibling).start()

    def forward_strip(k):
        received(s_v.at[k, me], s_recv_sem.at[k, 0])
        for landed in (s_v.at[k, from_y, first], s_v.at[k, from_cross, second]):
            remote(landed, landed, s_send_sem, s_recv_sem.at[k, 1], sibling).start()

    def strip_here(k):
        received(s_v.at[k, 0:2], s_recv_sem.at[k, 1])

    @pl.when(jnp.logical_and(z > 0, z < deep - 1))
    def _():
        pl.semaphore_wait(barrier, len(partners) + 2)

    @pl.when(jnp.logical_or(z == 0, z == deep - 1))
    def _():
        pl.semaphore_wait(barrier, len(partners) + 1)

    send_strip(0)

    @pl.when(z == deep - 2)
    def _():
        pl.semaphore_signal(hello.at[0], inc=1, device_id=below, device_id_type=MESH)

    @pl.when(z == 1)
    def _():
        pl.semaphore_signal(hello.at[1], inc=1, device_id=above, device_id_type=MESH)

    span = WIDE * CORES * 2 * rows

    orders = ORDERS.get(deep) or [[p for p in range(deep) if p != own] for own in range(deep)]

    def plane(n):
        if n == deep - 1:
            return z
        there = jnp.int32(0)
        for own in range(deep):
            there = jnp.where(z == own, orders[own][n], there)
        return there

    def turn(n):
        part = x_v[:, pl.ds(pl.multiple_of(plane(n) * span, span), span)].T
        for xx in range(WIDE):
            for cy in range(CORES * 2):
                start = (xx * CORES * 2 + cy) * rows
                if n == 0:
                    lead_tx[cy, xx * rows:(xx + 1) * rows, :] = part[start:start + rows, :]
                    continue
                for h in range(HALVES):
                    top = start + h * part_rows
                    tx[(n - 1) * HALVES + h, cy, xx * part_rows:(xx + 1) * part_rows, :] = part[top:top + part_rows, :]

    there_of = ((y_peer, from_y), (y_cross, from_cross), (sibling, from_sib))
    load_x.wait()
    turn(0)
    for device, there in there_of:
        remote(lead_tx.at[there], lead_rx.at[me], x_send_sem.at[0], x_recv_sem.at[pieces], device).start()
    for k in range(1, STRIPS):
        send_strip(k)
    lead_rx[me] = lead_tx[me]
    for n in range(1, deep):
        turn(n)
        for j in range((n - 1) * HALVES, n * HALVES):
            for device, there in there_of:
                remote(tx.at[j, there], rx.at[j, me], x_send_sem.at[1], x_recv_sem.at[j], device).start()
            rx[j, me] = tx[j, me]

    load_mask.wait()
    load_list.wait()
    scales = []
    for cc in range(CORES):
        here = (z * WIDE + wide) * CORES + cc
        mine = list_ref[here]
        tally = jnp.int32(0)
        for h in range(groups):
            tally = tally + jnp.where(list_ref[h] == mine, mask_ref[h], 0)
        done = jnp.full((1, wg_ref.shape[1]), mask_ref[here], jnp.int32).astype(jnp.float32)
        total = jnp.full((1, wg_ref.shape[1]), tally, jnp.int32).astype(jnp.float32)
        scales.append(done / (total + 1.0 - done))

    pltpu.make_async_copy(s_v.at[:, me], s_v.at[:, me], load_sem.at[1]).wait()
    load_w.wait()

    def grad(s_block):
        return lax.dot_general(
            s_block, w_v[...], (((1,), (1,)), ((), ())), preferred_element_type=jnp.float32
        ).astype(jnp.bfloat16)

    def joined(part):
        return jnp.concatenate([part(k) for k in range(STRIPS)], axis=1)

    own_columns = pl.ds(pl.multiple_of(y * half, half), half)
    ig_ref[:, own_columns] = grad(joined(lambda k: s_v[k, me]))

    def other_grad():
        block = [joined(lambda k: s_v[k, from_y, first]), joined(lambda k: s_v[k, from_cross, second])]
        ig_send[...] = grad(jnp.concatenate(block, axis=0))
        for tokens_of, device in ((first, y_peer), (second, y_cross)):
            remote(
                ig_send.at[tokens_of], ig_ref.at[tokens_of, own_columns], ig_send_sem, ig_recv_sem, device
            ).start()

    def product(lefts, rights, width):
        total = None
        for cc in range(CORES):
            left = jnp.concatenate([lefts(cc * 2), lefts(cc * 2 + 1)], axis=1)
            term = scales[cc][:, :width] * jnp.dot(left, rights(cc), preferred_element_type=jnp.float32)
            total = term if total is None else total + term
        return total

    def lead_partial(k):
        total = product(
            lambda cy: lead_rx[cy], lambda cc: s_v[k, cc * 2:cc * 2 + 2].reshape(2 * tokens, strip), strip
        )
        lead_part[k, 0] = total[:rows]
        lead_part[k, 1] = total[rows:]
        lead_send[k], lead_scale[k] = encode(lead_part[k, 1 - wide])
        remote(lead_send.at[k], lead_recv.at[k], px_send_sem.at[0], lead_recv_sem.at[k, 0], x_peer).start()
        remote(lead_scale.at[k], lead_rscale.at[k], px_send_sem.at[1], lead_recv_sem.at[k, 1], x_peer).start()

    def lead_gather(k):
        received(lead_recv.at[k], lead_recv_sem.at[k, 0])
        received(lead_rscale.at[k], lead_recv_sem.at[k, 1])
        coded, scale = encode(lead_part[k, wide] + decoded(lead_recv[k], lead_rscale[k]))
        for h in range(HALVES):
            lead_q[k, h] = coded[h * part_rows:(h + 1) * part_rows]
            lead_qscale[k, h] = scale
        there = at(plane(0), wide, core, y)
        for slot, (src, dst) in enumerate(((lead_q, zr), (lead_qscale, zr_scale))):
            remote(
                src.at[k], dst.at[z, :, :, columns[k]], z_send_sem.at[slot], z_recv_sem.at[z, slot], there
            ).start()

    def partial(j):
        received(rx.at[j, 0:3], x_recv_sem.at[j])
        total = product(
            lambda cy: rx[j, cy],
            lambda cc: joined(lambda k: s_v[k, cc * 2:cc * 2 + 2].reshape(2 * tokens, strip)),
            s_hbm.shape[1],
        )
        own_part[j, 0] = total[:part_rows]
        own_part[j, 1] = total[part_rows:]
        px_send[j], px_scale[j] = encode(own_part[j, 1 - wide])
        remote(px_send.at[j], px_recv.at[j], px_send_sem.at[2], px_recv_sem.at[j, 0], x_peer).start()
        remote(px_scale.at[j], px_rscale.at[j], px_send_sem.at[3], px_recv_sem.at[j, 1], x_peer).start()

    def gather(j):
        n, h = 1 + j // HALVES, j % HALVES
        received(px_recv.at[j], px_recv_sem.at[j, 0])
        received(px_rscale.at[j], px_recv_sem.at[j, 1])
        value = own_part[j, wide] + decoded(px_recv[j], px_rscale[j])
        if n == deep - 1:
            q[h] = value
            return
        q_send[j], q_scale[j] = encode(value)
        there = at(plane(n), wide, core, y)
        remote(q_send.at[j], zr.at[z, h], z_send_sem.at[2], z_recv_sem.at[z, 0], there).start()
        remote(q_scale.at[j], zr_scale.at[z, h], z_send_sem.at[3], z_recv_sem.at[z, 1], there).start()

    @pl.when(jnp.logical_and(z > 0, z < deep - 2))
    def _():
        pl.semaphore_wait(hello.at[0], 1)
        pl.semaphore_signal(hello.at[0], inc=1, device_id=below, device_id_type=MESH)

    @pl.when(jnp.logical_and(z > 1, z < deep - 1))
    def _():
        pl.semaphore_wait(hello.at[1], 1)
        pl.semaphore_signal(hello.at[1], inc=1, device_id=above, device_id_type=MESH)

    forward_strip(0)
    strip_here(0)
    received(lead_rx.at[0:3], x_recv_sem.at[pieces])
    lead_partial(0)
    forward_strip(1)
    for k in range(1, STRIPS - 1):
        forward_strip(k + 1)
        strip_here(k)
        lead_partial(k)

    @pl.when(z == 0)
    def _():
        pl.semaphore_wait(hello.at[0], 1)

    @pl.when(z == deep - 1)
    def _():
        pl.semaphore_wait(hello.at[1], 1)

    lead_gather(0)
    strip_here(STRIPS - 1)
    lead_partial(STRIPS - 1)
    other_grad()

    steps = [functools.partial(lead_gather, k) for k in range(1, STRIPS)]
    steps += [functools.partial(gather, j) for j in range(pieces)]
    for j in range(pieces):
        partial(j)
        if j >= LAG:
            steps.pop(0)()
    for step in steps:
        step()

    sent(s_v.at[:, 0:3], s_send_sem)
    sent(lead_tx.at[0:3], x_send_sem.at[0])
    sent(tx.at[:, 0:3], x_send_sem.at[1])
    for slot, ref in enumerate((lead_send, lead_scale, px_send, px_scale)):
        sent(ref, px_send_sem.at[slot])
    for slot, ref in enumerate((lead_q, lead_qscale, q_send, q_scale)):
        sent(ref, z_send_sem.at[slot])
    sent(ig_send, ig_send_sem)

    for n in range(deep - 1):
        source = jnp.where(n < z, n, n + 1)
        received(zr.at[source], z_recv_sem.at[source, 0])
        received(zr_scale.at[source], z_recv_sem.at[source, 1])
        for h in range(HALVES):
            value = decoded(zr[source, h], zr_scale[source, h])
            if n < deep - 2:
                q[h] = q[h] + value
            else:
                wg_ref[h * part_rows:(h + 1) * part_rows, :] = q[h] + value

    received(ig_send, ig_recv_sem)


def write_out(ig_ref, wg_ref, ig_hbm, wg_hbm, sems):
    copies = [
        pltpu.make_async_copy(ig_ref, ig_hbm, sems.at[0]),
        pltpu.make_async_copy(wg_ref, wg_hbm, sems.at[1]),
    ]
    for copy in copies:
        copy.start()
    for copy in copies:
        copy.wait()


def kernel_shards(deep, rows, x, s, w, mask, plist):
    tokens, width = x.shape
    values = s.shape[1]
    f32, bf16, i16 = jnp.float32, jnp.bfloat16, jnp.int16
    dma = pltpu.SemaphoreType.DMA
    anywhere = pl.BlockSpec(memory_space=pl.ANY)
    part_rows, pieces, strip = rows // HALVES, (deep - 1) * HALVES, values // STRIPS
    on_chip = pl.pallas_call(
        functools.partial(kernel, deep),
        out_shape=(
            pltpu.VMEM((tokens, width), bf16),
            pltpu.VMEM((rows, values), f32),
        ),
        in_specs=[anywhere] * 5,
        out_specs=(pl.BlockSpec(memory_space=pltpu.VMEM),) * 2,
        scratch_shapes=[
            pltpu.SMEM(mask.shape, jnp.int32),
            pltpu.SMEM(plist.shape, jnp.int32),
            pltpu.VMEM((tokens, width), bf16),
            pltpu.VMEM((STRIPS, CORES * 2, tokens, strip), bf16),
            pltpu.VMEM(w.shape, bf16),
            pltpu.VMEM((CORES * 2, WIDE * rows, tokens), bf16),
            pltpu.VMEM((CORES * 2, WIDE * rows, tokens), bf16),
            pltpu.VMEM((pieces, CORES * 2, WIDE * part_rows, tokens), bf16),
            pltpu.VMEM((pieces, CORES * 2, WIDE * part_rows, tokens), bf16),
            pltpu.VMEM((STRIPS, WIDE, rows, strip), f32),
            pltpu.VMEM((STRIPS, rows, strip), i16),
            pltpu.VMEM((STRIPS, 1, strip), f32),
            pltpu.VMEM((STRIPS, rows, strip), i16),
            pltpu.VMEM((STRIPS, 1, strip), f32),
            pltpu.VMEM((STRIPS, HALVES, part_rows, strip), i16),
            pltpu.VMEM((STRIPS, HALVES, 1, strip), f32),
            pltpu.VMEM((pieces, WIDE, part_rows, values), f32),
            pltpu.VMEM((pieces, part_rows, values), i16),
            pltpu.VMEM((pieces, 1, values), f32),
            pltpu.VMEM((pieces, part_rows, values), i16),
            pltpu.VMEM((pieces, 1, values), f32),
            pltpu.VMEM((HALVES, part_rows, values), f32),
            pltpu.VMEM((pieces - HALVES, part_rows, values), i16),
            pltpu.VMEM((pieces - HALVES, 1, values), f32),
            pltpu.VMEM((deep, HALVES, part_rows, values), i16),
            pltpu.VMEM((deep, HALVES, 1, values), f32),
            pltpu.VMEM((tokens, w.shape[0]), bf16),
            dma((5,)), dma, dma((STRIPS, 2)), dma((2,)), dma((pieces + 1,)),
            dma((4,)), dma((STRIPS, 2)), dma((pieces, 2)), dma((4,)), dma((deep, 2)), dma, dma,
            pltpu.SemaphoreType.REGULAR((2,)),
        ],
        compiler_params=pltpu.CompilerParams(collective_id=0, has_side_effects=True),
    )(mask, plist, x, s, w)
    return pl.pallas_call(
        write_out,
        out_shape=(
            jax.ShapeDtypeStruct((tokens, width), bf16),
            jax.ShapeDtypeStruct((rows, values), f32),
        ),
        in_specs=[pl.BlockSpec(memory_space=pltpu.VMEM)] * 2,
        out_specs=(anywhere,) * 2,
        scratch_shapes=[dma((2,))],
        compiler_params=pltpu.CompilerParams(vmem_limit_bytes=SMALL),
    )(*(pltpu.with_memory_space_constraint(part, pltpu.VMEM) for part in on_chip))


def solution(mesh):
    outer, inner = mesh.shape["grp"], mesh.shape["fsdp"]

    def shards(x, s, w, mask, plist):
        rows = x.shape[1] // (outer * inner)
        if inner == 2 and outer % (CORES * WIDE) == 0 and outer // (CORES * WIDE) >= 4 and rows % (16 * HALVES) == 0 and x.shape[0] % 128 == 0 and s.shape[1] % (128 * STRIPS) == 0:
            return tuple(kernel_shards(outer // (CORES * WIDE), rows, x, s, w, mask, plist))
        return collective_shards(x, s, w, mask, plist)

    in_specs = (P(("grp", "fsdp"), None), P(("grp", "fsdp"), None), P("fsdp", None), P(), P())
    out_specs = (P(("grp", "fsdp"), None), P(("grp", "fsdp"), None))
    return jax.shard_map(shards, mesh=mesh, in_specs=in_specs, out_specs=out_specs, check_vma=False)
```

```python
import functools

import jax
import jax.numpy as jnp
from jax import lax
from jax.experimental import pallas as pl
from jax.experimental.pallas import tpu as pltpu
from jax.sharding import PartitionSpec as P

MESH = pl.DeviceIdType.MESH
CORES = 2
WIDE = 2
HALVES = 2
STRIPS = 4
LAG = 1
GRAD_AFTER = 1
ORDERS = {4: ((3, 2, 1), (0, 3, 2), (0, 3, 1), (0, 1, 2))}
SMALL = 1 << 20
STEPS = 32766.0
TINY = 1e-33


def collective_shards(
    normalized_inputs,
    output_sensitivity,
    projection_weights,
    completion_mask,
    replica_partition_list,
):
    replica_index = lax.axis_index("grp")
    selected_replica = lax.iota(jnp.int32, completion_mask.shape[0]) == replica_index
    assigned_piece = jnp.sum(jnp.where(selected_replica, replica_partition_list, 0))
    finished_indicator = jnp.sum(jnp.where(selected_replica, completion_mask, 0))
    finisher_tally = jnp.sum(
        jnp.where(replica_partition_list == assigned_piece, completion_mask, 0)
    )
    living_float = finished_indicator.astype(jnp.float32)
    decode_sum = living_float / (finisher_tally.astype(jnp.float32) + 1.0 - living_float)
    tokens_here = normalized_inputs.shape[0]
    model_width = normalized_inputs.shape[1]
    inner_size = lax.axis_size("fsdp")
    outer_size = lax.axis_size("grp")
    input_grad = lax.dot_general(
        output_sensitivity,
        lax.all_gather(projection_weights, "fsdp", axis=0, tiled=True),
        (((1,), (1,)), ((), ())),
        preferred_element_type=jnp.float32,
    ).astype(jnp.bfloat16)
    owner_rows = model_width // (outer_size * inner_size)
    reordered = normalized_inputs.reshape(tokens_here, outer_size, inner_size, owner_rows)
    reordered = reordered.transpose(0, 2, 1, 3).reshape(tokens_here, model_width)
    column_block = lax.all_to_all(reordered, "fsdp", split_axis=1, concat_axis=0, tiled=True)
    group_block = lax.dot_general(
        column_block,
        lax.all_gather(output_sensitivity, "fsdp", axis=0, tiled=True),
        (((0,), (0,)), ((), ())),
        preferred_element_type=jnp.float32,
    )
    weight_grad = lax.psum_scatter(decode_sum * group_block, "grp", scatter_dimension=0, tiled=True)
    return (input_grad, weight_grad)


def encode(value):
    top = jnp.maximum(jnp.max(jnp.abs(value), axis=0, keepdims=True), TINY)
    coded = jnp.round(value * (STEPS / top)).astype(jnp.int32).astype(jnp.int16)
    return coded, top * (1.0 / STEPS)


def decoded(coded, step):
    return coded.astype(jnp.int32).astype(jnp.float32) * step


def kernel(
    deep,
    mask_hbm, list_hbm, x_hbm, s_hbm, w_hbm,
    ig_ref, wg_ref,
    mask_ref, list_ref,
    x_v, s_v, w_v, lead_tx, lead_rx, tx, rx,
    lead_part, lead_send, lead_scale, lead_recv, lead_rscale, lead_q, lead_qscale,
    own_part, px_send, px_scale, px_recv, px_rscale, q, q_send, q_scale, zr, zr_scale, ig_send,
    load_sem, s_send_sem, s_recv_sem, x_send_sem, x_recv_sem,
    px_send_sem, lead_recv_sem, px_recv_sem, z_send_sem, z_recv_sem, ig_send_sem, ig_recv_sem, hello,
):
    grp = lax.axis_index("grp")
    y = lax.axis_index("fsdp")
    core = lax.rem(grp, CORES)
    wide = lax.rem(grp // CORES, WIDE)
    z = grp // (CORES * WIDE)
    oy, oc = 1 - y, 1 - core
    tokens = s_hbm.shape[0]
    groups = mask_ref.shape[0]
    rows = wg_ref.shape[0]
    half = w_hbm.shape[0]
    part_tokens = tokens // 2
    part_rows = rows // HALVES
    pieces = (deep - 1) * HALVES
    strip = s_hbm.shape[1] // STRIPS

    def at(zz, xx, cc, yy):
        return ((zz * WIDE + xx) * CORES + cc, yy)

    def remote(src, dst, send, recv, device):
        return pltpu.make_async_remote_copy(
            src_ref=src, dst_ref=dst, send_sem=send, recv_sem=recv,
            device_id=device, device_id_type=MESH,
        )

    y_peer = at(z, wide, core, oy)
    y_cross = at(z, wide, oc, oy)
    sibling = at(z, wide, oc, y)
    x_peer = at(z, 1 - wide, core, y)
    below = at(lax.rem(z + deep - 1, deep), wide, core, y)
    above = at(lax.rem(z + 1, deep), wide, core, y)
    me = core * 2 + y
    from_y = core * 2 + oy
    from_cross = oc * 2 + oy
    from_sib = oc * 2 + y

    barrier = pltpu.get_barrier_semaphore()
    partners = [y_peer, y_cross, sibling, x_peer]
    for partner in partners:
        pl.semaphore_signal(barrier, inc=1, device_id=partner, device_id_type=MESH)

    @pl.when(z > 0)
    def _():
        pl.semaphore_signal(barrier, inc=1, device_id=below, device_id_type=MESH)

    @pl.when(z < deep - 1)
    def _():
        pl.semaphore_signal(barrier, inc=1, device_id=above, device_id_type=MESH)

    load_x = pltpu.make_async_copy(x_hbm, x_v, load_sem.at[0])
    load_w = pltpu.make_async_copy(w_hbm, w_v, load_sem.at[2])
    load_mask = pltpu.make_async_copy(mask_hbm, mask_ref, load_sem.at[3])
    load_list = pltpu.make_async_copy(list_hbm, list_ref, load_sem.at[4])
    columns = [pl.ds(k * strip, strip) for k in range(STRIPS)]
    load_x.start()
    for k in range(STRIPS):
        pltpu.make_async_copy(s_hbm.at[:, columns[k]], s_v.at[k, me], load_sem.at[1]).start()
    load_w.start()
    load_mask.start()
    load_list.start()

    first, second = pl.ds(0, part_tokens), pl.ds(part_tokens, part_tokens)
    def received(ref, sem):
        remote(ref, ref, sem, sem, sibling).wait_recv()

    def sent(ref, sem):
        remote(ref, ref, sem, sem, sibling).wait_send()

    def send_strip(k):
        own = s_v.at[k, me]
        remote(s_hbm.at[first, columns[k]], own.at[first], s_send_sem, s_recv_sem.at[k, 0], y_peer).start()
        remote(s_hbm.at[second, columns[k]], own.at[second], s_send_sem, s_recv_sem.at[k, 0], y_cross).start()
        remote(s_hbm.at[:, columns[k]], own, s_send_sem, s_recv_sem.at[k, 1], sibling).start()

    def forward_strip(k):
        received(s_v.at[k, me], s_recv_sem.at[k, 0])
        for landed in (s_v.at[k, from_y, first], s_v.at[k, from_cross, second]):
            remote(landed, landed, s_send_sem, s_recv_sem.at[k, 1], sibling).start()

    def strip_here(k):
        received(s_v.at[k, 0:2], s_recv_sem.at[k, 1])

    @pl.when(jnp.logical_and(z > 0, z < deep - 1))
    def _():
        pl.semaphore_wait(barrier, len(partners) + 2)

    @pl.when(jnp.logical_or(z == 0, z == deep - 1))
    def _():
        pl.semaphore_wait(barrier, len(partners) + 1)

    send_strip(0)

    @pl.when(z == deep - 2)
    def _():
        pl.semaphore_signal(hello.at[0], inc=1, device_id=below, device_id_type=MESH)

    @pl.when(z == 1)
    def _():
        pl.semaphore_signal(hello.at[1], inc=1, device_id=above, device_id_type=MESH)

    span = WIDE * CORES * 2 * rows

    orders = ORDERS.get(deep) or [[p for p in range(deep) if p != own] for own in range(deep)]

    def plane(n):
        if n == deep - 1:
            return z
        there = jnp.int32(0)
        for own in range(deep):
            there = jnp.where(z == own, orders[own][n], there)
        return there

    def turn(n):
        part = x_v[:, pl.ds(pl.multiple_of(plane(n) * span, span), span)].T
        for xx in range(WIDE):
            for cy in range(CORES * 2):
                start = (xx * CORES * 2 + cy) * rows
                if n == 0:
                    lead_tx[cy, xx * rows:(xx + 1) * rows, :] = part[start:start + rows, :]
                    continue
                for h in range(HALVES):
                    top = start + h * part_rows
                    tx[(n - 1) * HALVES + h, cy, xx * part_rows:(xx + 1) * part_rows, :] = part[top:top + part_rows, :]

    there_of = ((y_peer, from_y), (y_cross, from_cross), (sibling, from_sib))
    load_x.wait()
    turn(0)
    for device, there in there_of:
        remote(lead_tx.at[there], lead_rx.at[me], x_send_sem.at[0], x_recv_sem.at[pieces], device).start()
    for k in range(1, STRIPS):
        send_strip(k)
    lead_rx[me] = lead_tx[me]
    for n in range(1, deep):
        turn(n)
        for j in range((n - 1) * HALVES, n * HALVES):
            for device, there in there_of:
                remote(tx.at[j, there], rx.at[j, me], x_send_sem.at[1], x_recv_sem.at[j], device).start()
            rx[j, me] = tx[j, me]

    load_mask.wait()
    load_list.wait()
    scales = []
    for cc in range(CORES):
        here = (z * WIDE + wide) * CORES + cc
        mine = list_ref[here]
        tally = jnp.int32(0)
        for h in range(groups):
            tally = tally + jnp.where(list_ref[h] == mine, mask_ref[h], 0)
        done = jnp.full((1, wg_ref.shape[1]), mask_ref[here], jnp.int32).astype(jnp.float32)
        total = jnp.full((1, wg_ref.shape[1]), tally, jnp.int32).astype(jnp.float32)
        scales.append(done / (total + 1.0 - done))

    pltpu.make_async_copy(s_v.at[:, me], s_v.at[:, me], load_sem.at[1]).wait()
    load_w.wait()

    def grad(s_block):
        return lax.dot_general(
            s_block, w_v[...], (((1,), (1,)), ((), ())), preferred_element_type=jnp.float32
        ).astype(jnp.bfloat16)

    def joined(part):
        return jnp.concatenate([part(k) for k in range(STRIPS)], axis=1)

    own_columns = pl.ds(pl.multiple_of(y * half, half), half)
    ig_ref[:, own_columns] = grad(joined(lambda k: s_v[k, me]))

    def other_grad():
        block = [joined(lambda k: s_v[k, from_y, first]), joined(lambda k: s_v[k, from_cross, second])]
        ig_send[...] = grad(jnp.concatenate(block, axis=0))
        for tokens_of, device in ((first, y_peer), (second, y_cross)):
            remote(
                ig_send.at[tokens_of], ig_ref.at[tokens_of, own_columns], ig_send_sem, ig_recv_sem, device
            ).start()

    def product(lefts, rights, width):
        total = None
        for cc in range(CORES):
            left = jnp.concatenate([lefts(cc * 2), lefts(cc * 2 + 1)], axis=1)
            term = scales[cc][:, :width] * jnp.dot(left, rights(cc), preferred_element_type=jnp.float32)
            total = term if total is None else total + term
        return total

    def lead_partial(k):
        total = product(
            lambda cy: lead_rx[cy], lambda cc: s_v[k, cc * 2:cc * 2 + 2].reshape(2 * tokens, strip), strip
        )
        lead_part[k, 0] = total[:rows]
        lead_part[k, 1] = total[rows:]
        lead_send[k], lead_scale[k] = encode(lead_part[k, 1 - wide])
        remote(lead_scale.at[k], lead_rscale.at[k], px_send_sem.at[1], lead_recv_sem.at[k, 1], x_peer).start()
        remote(lead_send.at[k], lead_recv.at[k], px_send_sem.at[0], lead_recv_sem.at[k, 0], x_peer).start()

    def lead_gather(k):
        received(lead_recv.at[k], lead_recv_sem.at[k, 0])
        received(lead_rscale.at[k], lead_recv_sem.at[k, 1])
        coded, scale = encode(lead_part[k, wide] + decoded(lead_recv[k], lead_rscale[k]))
        for h in range(HALVES):
            lead_q[k, h] = coded[h * part_rows:(h + 1) * part_rows]
            lead_qscale[k, h] = scale
        there = at(plane(0), wide, core, y)
        for slot, (src, dst) in ((1, (lead_qscale, zr_scale)), (0, (lead_q, zr))):
            remote(
                src.at[k], dst.at[z, :, :, columns[k]], z_send_sem.at[slot], z_recv_sem.at[z, slot], there
            ).start()

    def partial(j):
        received(rx.at[j, 0:3], x_recv_sem.at[j])
        total = product(
            lambda cy: rx[j, cy],
            lambda cc: joined(lambda k: s_v[k, cc * 2:cc * 2 + 2].reshape(2 * tokens, strip)),
            s_hbm.shape[1],
        )
        own_part[j, 0] = total[:part_rows]
        own_part[j, 1] = total[part_rows:]
        px_send[j], px_scale[j] = encode(own_part[j, 1 - wide])
        remote(px_scale.at[j], px_rscale.at[j], px_send_sem.at[3], px_recv_sem.at[j, 1], x_peer).start()
        remote(px_send.at[j], px_recv.at[j], px_send_sem.at[2], px_recv_sem.at[j, 0], x_peer).start()

    def gather(j):
        n, h = 1 + j // HALVES, j % HALVES
        received(px_recv.at[j], px_recv_sem.at[j, 0])
        received(px_rscale.at[j], px_recv_sem.at[j, 1])
        value = own_part[j, wide] + decoded(px_recv[j], px_rscale[j])
        if n == deep - 1:
            q[h] = value
            return
        q_send[j], q_scale[j] = encode(value)
        there = at(plane(n), wide, core, y)
        remote(q_scale.at[j], zr_scale.at[z, h], z_send_sem.at[3], z_recv_sem.at[z, 1], there).start()
        remote(q_send.at[j], zr.at[z, h], z_send_sem.at[2], z_recv_sem.at[z, 0], there).start()

    @pl.when(jnp.logical_and(z > 0, z < deep - 2))
    def _():
        pl.semaphore_wait(hello.at[0], 1)
        pl.semaphore_signal(hello.at[0], inc=1, device_id=below, device_id_type=MESH)

    @pl.when(jnp.logical_and(z > 1, z < deep - 1))
    def _():
        pl.semaphore_wait(hello.at[1], 1)
        pl.semaphore_signal(hello.at[1], inc=1, device_id=above, device_id_type=MESH)

    forward_strip(0)
    strip_here(0)
    received(lead_rx.at[0:3], x_recv_sem.at[pieces])
    lead_partial(0)
    forward_strip(1)
    for k in range(1, STRIPS - 1):
        forward_strip(k + 1)
        strip_here(k)
        lead_partial(k)

    @pl.when(z == 0)
    def _():
        pl.semaphore_wait(hello.at[0], 1)

    @pl.when(z == deep - 1)
    def _():
        pl.semaphore_wait(hello.at[1], 1)

    lead_gather(0)
    strip_here(STRIPS - 1)
    lead_partial(STRIPS - 1)

    steps = [functools.partial(lead_gather, k) for k in range(1, STRIPS)]
    steps += [functools.partial(gather, j) for j in range(pieces)]
    for j in range(pieces):
        partial(j)
        if j == GRAD_AFTER:
            other_grad()
        if j >= LAG:
            steps.pop(0)()
    for step in steps:
        step()

    sent(s_v.at[:, 0:3], s_send_sem)
    sent(lead_tx.at[0:3], x_send_sem.at[0])
    sent(tx.at[:, 0:3], x_send_sem.at[1])
    for slot, ref in enumerate((lead_send, lead_scale, px_send, px_scale)):
        sent(ref, px_send_sem.at[slot])

    for n in range(deep - 1):
        source = jnp.where(n < z, n, n + 1)
        received(zr.at[source], z_recv_sem.at[source, 0])
        received(zr_scale.at[source], z_recv_sem.at[source, 1])
        for h in range(HALVES):
            value = decoded(zr[source, h], zr_scale[source, h])
            if n < deep - 2:
                q[h] = q[h] + value
            else:
                wg_ref[h * part_rows:(h + 1) * part_rows, :] = q[h] + value

    received(ig_send, ig_recv_sem)
    for slot, ref in enumerate((lead_q, lead_qscale, q_send, q_scale)):
        sent(ref, z_send_sem.at[slot])
    sent(ig_send, ig_send_sem)


def write_out(ig_ref, wg_ref, ig_hbm, wg_hbm, sems):
    copies = [
        pltpu.make_async_copy(ig_ref, ig_hbm, sems.at[0]),
        pltpu.make_async_copy(wg_ref, wg_hbm, sems.at[1]),
    ]
    for copy in copies:
        copy.start()
    for copy in copies:
        copy.wait()


def kernel_shards(deep, rows, x, s, w, mask, plist):
    tokens, width = x.shape
    values = s.shape[1]
    f32, bf16, i16 = jnp.float32, jnp.bfloat16, jnp.int16
    dma = pltpu.SemaphoreType.DMA
    anywhere = pl.BlockSpec(memory_space=pl.ANY)
    part_rows, pieces, strip = rows // HALVES, (deep - 1) * HALVES, values // STRIPS
    on_chip = pl.pallas_call(
        functools.partial(kernel, deep),
        out_shape=(
            pltpu.VMEM((tokens, width), bf16),
            pltpu.VMEM((rows, values), f32),
        ),
        in_specs=[anywhere] * 5,
        out_specs=(pl.BlockSpec(memory_space=pltpu.VMEM),) * 2,
        scratch_shapes=[
            pltpu.SMEM(mask.shape, jnp.int32),
            pltpu.SMEM(plist.shape, jnp.int32),
            pltpu.VMEM((tokens, width), bf16),
            pltpu.VMEM((STRIPS, CORES * 2, tokens, strip), bf16),
            pltpu.VMEM(w.shape, bf16),
            pltpu.VMEM((CORES * 2, WIDE * rows, tokens), bf16),
            pltpu.VMEM((CORES * 2, WIDE * rows, tokens), bf16),
            pltpu.VMEM((pieces, CORES * 2, WIDE * part_rows, tokens), bf16),
            pltpu.VMEM((pieces, CORES * 2, WIDE * part_rows, tokens), bf16),
            pltpu.VMEM((STRIPS, WIDE, rows, strip), f32),
            pltpu.VMEM((STRIPS, rows, strip), i16),
            pltpu.VMEM((STRIPS, 1, strip), f32),
            pltpu.VMEM((STRIPS, rows, strip), i16),
            pltpu.VMEM((STRIPS, 1, strip), f32),
            pltpu.VMEM((STRIPS, HALVES, part_rows, strip), i16),
            pltpu.VMEM((STRIPS, HALVES, 1, strip), f32),
            pltpu.VMEM((pieces, WIDE, part_rows, values), f32),
            pltpu.VMEM((pieces, part_rows, values), i16),
            pltpu.VMEM((pieces, 1, values), f32),
            pltpu.VMEM((pieces, part_rows, values), i16),
            pltpu.VMEM((pieces, 1, values), f32),
            pltpu.VMEM((HALVES, part_rows, values), f32),
            pltpu.VMEM((pieces - HALVES, part_rows, values), i16),
            pltpu.VMEM((pieces - HALVES, 1, values), f32),
            pltpu.VMEM((deep, HALVES, part_rows, values), i16),
            pltpu.VMEM((deep, HALVES, 1, values), f32),
            pltpu.VMEM((tokens, w.shape[0]), bf16),
            dma((5,)), dma, dma((STRIPS, 2)), dma((2,)), dma((pieces + 1,)),
            dma((4,)), dma((STRIPS, 2)), dma((pieces, 2)), dma((4,)), dma((deep, 2)), dma, dma,
            pltpu.SemaphoreType.REGULAR((2,)),
        ],
        compiler_params=pltpu.CompilerParams(collective_id=0, has_side_effects=True),
    )(mask, plist, x, s, w)
    return pl.pallas_call(
        write_out,
        out_shape=(
            jax.ShapeDtypeStruct((tokens, width), bf16),
            jax.ShapeDtypeStruct((rows, values), f32),
        ),
        in_specs=[pl.BlockSpec(memory_space=pltpu.VMEM)] * 2,
        out_specs=(anywhere,) * 2,
        scratch_shapes=[dma((2,))],
        compiler_params=pltpu.CompilerParams(vmem_limit_bytes=SMALL),
    )(*(pltpu.with_memory_space_constraint(part, pltpu.VMEM) for part in on_chip))


def solution(mesh):
    outer, inner = mesh.shape["grp"], mesh.shape["fsdp"]

    def shards(x, s, w, mask, plist):
        rows = x.shape[1] // (outer * inner)
        if inner == 2 and outer % (CORES * WIDE) == 0 and outer // (CORES * WIDE) >= 4 and rows % (16 * HALVES) == 0 and x.shape[0] % 128 == 0 and s.shape[1] % (128 * STRIPS) == 0:
            return tuple(kernel_shards(outer // (CORES * WIDE), rows, x, s, w, mask, plist))
        return collective_shards(x, s, w, mask, plist)

    in_specs = (P(("grp", "fsdp"), None), P(("grp", "fsdp"), None), P("fsdp", None), P(), P())
    out_specs = (P(("grp", "fsdp"), None), P(("grp", "fsdp"), None))
    return jax.shard_map(shards, mesh=mesh, in_specs=in_specs, out_specs=out_specs, check_vma=False)
```

```python
import functools

import jax
import jax.numpy as jnp
from jax import lax
from jax.experimental import pallas as pl
from jax.experimental.pallas import tpu as pltpu
from jax.sharding import PartitionSpec as P

MESH = pl.DeviceIdType.MESH
CORES = 2
WIDE = 2
HALVES = 2
STRIPS = 4
LAG = 1
GRAD_AFTER = 1
ORDERS = {4: ((3, 2, 1), (0, 3, 2), (0, 3, 1), (0, 1, 2))}
SMALL = 1 << 21
STEPS = 32766.0
TINY = 1e-33


def collective_shards(
    normalized_inputs,
    output_sensitivity,
    projection_weights,
    completion_mask,
    replica_partition_list,
):
    replica_index = lax.axis_index("grp")
    selected_replica = lax.iota(jnp.int32, completion_mask.shape[0]) == replica_index
    assigned_piece = jnp.sum(jnp.where(selected_replica, replica_partition_list, 0))
    finished_indicator = jnp.sum(jnp.where(selected_replica, completion_mask, 0))
    finisher_tally = jnp.sum(
        jnp.where(replica_partition_list == assigned_piece, completion_mask, 0)
    )
    living_float = finished_indicator.astype(jnp.float32)
    decode_sum = living_float / (finisher_tally.astype(jnp.float32) + 1.0 - living_float)
    tokens_here = normalized_inputs.shape[0]
    model_width = normalized_inputs.shape[1]
    inner_size = lax.axis_size("fsdp")
    outer_size = lax.axis_size("grp")
    input_grad = lax.dot_general(
        output_sensitivity,
        lax.all_gather(projection_weights, "fsdp", axis=0, tiled=True),
        (((1,), (1,)), ((), ())),
        preferred_element_type=jnp.float32,
    ).astype(jnp.bfloat16)
    owner_rows = model_width // (outer_size * inner_size)
    reordered = normalized_inputs.reshape(tokens_here, outer_size, inner_size, owner_rows)
    reordered = reordered.transpose(0, 2, 1, 3).reshape(tokens_here, model_width)
    column_block = lax.all_to_all(reordered, "fsdp", split_axis=1, concat_axis=0, tiled=True)
    group_block = lax.dot_general(
        column_block,
        lax.all_gather(output_sensitivity, "fsdp", axis=0, tiled=True),
        (((0,), (0,)), ((), ())),
        preferred_element_type=jnp.float32,
    )
    weight_grad = lax.psum_scatter(decode_sum * group_block, "grp", scatter_dimension=0, tiled=True)
    return (input_grad, weight_grad)


def encode(value):
    top = jnp.maximum(jnp.max(jnp.abs(value), axis=0, keepdims=True), TINY)
    coded = jnp.round(value * (STEPS / top)).astype(jnp.int32).astype(jnp.int16)
    return coded, top * (1.0 / STEPS)


def decoded(coded, step):
    return coded.astype(jnp.int32).astype(jnp.float32) * step


def kernel(
    deep,
    mask_hbm, list_hbm, x_hbm, s_hbm, w_hbm,
    ig_ref, q, zr, zr_scale,
    mask_ref, list_ref,
    x_v, s_v, w_v, lead_tx, lead_rx, tx, rx,
    lead_part, lead_send, lead_scale, lead_recv, lead_rscale, lead_q, lead_qscale,
    own_part, px_send, px_scale, px_recv, px_rscale, q_send, q_scale, ig_send,
    load_sem, s_send_sem, s_recv_sem, x_send_sem, x_recv_sem,
    px_send_sem, lead_recv_sem, px_recv_sem, z_send_sem, z_recv_sem, ig_send_sem, ig_recv_sem, hello,
):
    grp = lax.axis_index("grp")
    y = lax.axis_index("fsdp")
    core = lax.rem(grp, CORES)
    wide = lax.rem(grp // CORES, WIDE)
    z = grp // (CORES * WIDE)
    oy, oc = 1 - y, 1 - core
    tokens = s_hbm.shape[0]
    groups = mask_ref.shape[0]
    rows = q.shape[0] * q.shape[1]
    half = w_hbm.shape[0]
    part_tokens = tokens // 2
    part_rows = rows // HALVES
    pieces = (deep - 1) * HALVES
    strip = s_hbm.shape[1] // STRIPS

    def at(zz, xx, cc, yy):
        return ((zz * WIDE + xx) * CORES + cc, yy)

    def remote(src, dst, send, recv, device):
        return pltpu.make_async_remote_copy(
            src_ref=src, dst_ref=dst, send_sem=send, recv_sem=recv,
            device_id=device, device_id_type=MESH,
        )

    y_peer = at(z, wide, core, oy)
    y_cross = at(z, wide, oc, oy)
    sibling = at(z, wide, oc, y)
    x_peer = at(z, 1 - wide, core, y)
    below = at(lax.rem(z + deep - 1, deep), wide, core, y)
    above = at(lax.rem(z + 1, deep), wide, core, y)
    me = core * 2 + y
    from_y = core * 2 + oy
    from_cross = oc * 2 + oy
    from_sib = oc * 2 + y

    barrier = pltpu.get_barrier_semaphore()
    partners = [y_peer, y_cross, sibling, x_peer]
    for partner in partners:
        pl.semaphore_signal(barrier, inc=1, device_id=partner, device_id_type=MESH)

    @pl.when(z > 0)
    def _():
        pl.semaphore_signal(barrier, inc=1, device_id=below, device_id_type=MESH)

    @pl.when(z < deep - 1)
    def _():
        pl.semaphore_signal(barrier, inc=1, device_id=above, device_id_type=MESH)

    load_x = pltpu.make_async_copy(x_hbm, x_v, load_sem.at[0])
    load_w = pltpu.make_async_copy(w_hbm, w_v, load_sem.at[2])
    load_mask = pltpu.make_async_copy(mask_hbm, mask_ref, load_sem.at[3])
    load_list = pltpu.make_async_copy(list_hbm, list_ref, load_sem.at[4])
    columns = [pl.ds(k * strip, strip) for k in range(STRIPS)]
    load_x.start()
    for k in range(STRIPS):
        pltpu.make_async_copy(s_hbm.at[:, columns[k]], s_v.at[k, me], load_sem.at[1]).start()
    load_w.start()
    load_mask.start()
    load_list.start()

    first, second = pl.ds(0, part_tokens), pl.ds(part_tokens, part_tokens)
    def received(ref, sem):
        remote(ref, ref, sem, sem, sibling).wait_recv()

    def sent(ref, sem):
        remote(ref, ref, sem, sem, sibling).wait_send()

    def send_strip(k):
        own = s_v.at[k, me]
        remote(s_hbm.at[first, columns[k]], own.at[first], s_send_sem, s_recv_sem.at[k, 0], y_peer).start()
        remote(s_hbm.at[second, columns[k]], own.at[second], s_send_sem, s_recv_sem.at[k, 0], y_cross).start()
        remote(s_hbm.at[:, columns[k]], own, s_send_sem, s_recv_sem.at[k, 1], sibling).start()

    def forward_strip(k):
        received(s_v.at[k, me], s_recv_sem.at[k, 0])
        for landed in (s_v.at[k, from_y, first], s_v.at[k, from_cross, second]):
            remote(landed, landed, s_send_sem, s_recv_sem.at[k, 1], sibling).start()

    def strip_here(k):
        received(s_v.at[k, 0:2], s_recv_sem.at[k, 1])

    @pl.when(jnp.logical_and(z > 0, z < deep - 1))
    def _():
        pl.semaphore_wait(barrier, len(partners) + 2)

    @pl.when(jnp.logical_or(z == 0, z == deep - 1))
    def _():
        pl.semaphore_wait(barrier, len(partners) + 1)

    send_strip(0)

    @pl.when(z == deep - 2)
    def _():
        pl.semaphore_signal(hello.at[0], inc=1, device_id=below, device_id_type=MESH)

    @pl.when(z == 1)
    def _():
        pl.semaphore_signal(hello.at[1], inc=1, device_id=above, device_id_type=MESH)

    span = WIDE * CORES * 2 * rows

    orders = ORDERS.get(deep) or [[p for p in range(deep) if p != own] for own in range(deep)]

    def plane(n):
        if n == deep - 1:
            return z
        there = jnp.int32(0)
        for own in range(deep):
            there = jnp.where(z == own, orders[own][n], there)
        return there

    def turn(n):
        part = x_v[:, pl.ds(pl.multiple_of(plane(n) * span, span), span)].T
        for xx in range(WIDE):
            for cy in range(CORES * 2):
                start = (xx * CORES * 2 + cy) * rows
                if n == 0:
                    lead_tx[cy, xx * rows:(xx + 1) * rows, :] = part[start:start + rows, :]
                    continue
                for h in range(HALVES):
                    top = start + h * part_rows
                    tx[(n - 1) * HALVES + h, cy, xx * part_rows:(xx + 1) * part_rows, :] = part[top:top + part_rows, :]

    there_of = ((y_peer, from_y), (y_cross, from_cross), (sibling, from_sib))
    load_x.wait()
    turn(0)
    for device, there in there_of:
        remote(lead_tx.at[there], lead_rx.at[me], x_send_sem.at[0], x_recv_sem.at[pieces], device).start()
    for k in range(1, STRIPS):
        send_strip(k)
    lead_rx[me] = lead_tx[me]
    for n in range(1, deep):
        turn(n)
        for j in range((n - 1) * HALVES, n * HALVES):
            for device, there in there_of:
                remote(tx.at[j, there], rx.at[j, me], x_send_sem.at[1], x_recv_sem.at[j], device).start()
            rx[j, me] = tx[j, me]

    load_mask.wait()
    load_list.wait()
    scales = []
    for cc in range(CORES):
        here = (z * WIDE + wide) * CORES + cc
        mine = list_ref[here]
        tally = jnp.int32(0)
        for h in range(groups):
            tally = tally + jnp.where(list_ref[h] == mine, mask_ref[h], 0)
        done = jnp.full((1, s_hbm.shape[1]), mask_ref[here], jnp.int32).astype(jnp.float32)
        total = jnp.full((1, s_hbm.shape[1]), tally, jnp.int32).astype(jnp.float32)
        scales.append(done / (total + 1.0 - done))

    pltpu.make_async_copy(s_v.at[:, me], s_v.at[:, me], load_sem.at[1]).wait()
    load_w.wait()

    def grad(s_block):
        return lax.dot_general(
            s_block, w_v[...], (((1,), (1,)), ((), ())), preferred_element_type=jnp.float32
        ).astype(jnp.bfloat16)

    def joined(part):
        return jnp.concatenate([part(k) for k in range(STRIPS)], axis=1)

    zr[z] = jnp.zeros(zr.shape[1:], zr.dtype)
    zr_scale[z] = jnp.zeros(zr_scale.shape[1:], zr_scale.dtype)

    own_columns = pl.ds(pl.multiple_of(y * half, half), half)
    ig_ref[:, own_columns] = grad(joined(lambda k: s_v[k, me]))

    def other_grad():
        block = [joined(lambda k: s_v[k, from_y, first]), joined(lambda k: s_v[k, from_cross, second])]
        ig_send[...] = grad(jnp.concatenate(block, axis=0))
        for tokens_of, device in ((first, y_peer), (second, y_cross)):
            remote(
                ig_send.at[tokens_of], ig_ref.at[tokens_of, own_columns], ig_send_sem, ig_recv_sem, device
            ).start()

    def product(lefts, rights, width):
        total = None
        for cc in range(CORES):
            left = jnp.concatenate([lefts(cc * 2), lefts(cc * 2 + 1)], axis=1)
            term = scales[cc][:, :width] * jnp.dot(left, rights(cc), preferred_element_type=jnp.float32)
            total = term if total is None else total + term
        return total

    def lead_partial(k):
        total = product(
            lambda cy: lead_rx[cy], lambda cc: s_v[k, cc * 2:cc * 2 + 2].reshape(2 * tokens, strip), strip
        )
        lead_part[k, 0] = total[:rows]
        lead_part[k, 1] = total[rows:]
        lead_send[k], lead_scale[k] = encode(lead_part[k, 1 - wide])
        remote(lead_scale.at[k], lead_rscale.at[k], px_send_sem.at[1], lead_recv_sem.at[k, 1], x_peer).start()
        remote(lead_send.at[k], lead_recv.at[k], px_send_sem.at[0], lead_recv_sem.at[k, 0], x_peer).start()

    def lead_gather(k):
        received(lead_recv.at[k], lead_recv_sem.at[k, 0])
        received(lead_rscale.at[k], lead_recv_sem.at[k, 1])
        coded, scale = encode(lead_part[k, wide] + decoded(lead_recv[k], lead_rscale[k]))
        for h in range(HALVES):
            lead_q[k, h] = coded[h * part_rows:(h + 1) * part_rows]
            lead_qscale[k, h] = scale
        there = at(plane(0), wide, core, y)
        for slot, (src, dst) in ((1, (lead_qscale, zr_scale)), (0, (lead_q, zr))):
            remote(
                src.at[k], dst.at[z, :, :, columns[k]], z_send_sem.at[slot], z_recv_sem.at[z, slot], there
            ).start()

    def partial(j):
        received(rx.at[j, 0:3], x_recv_sem.at[j])
        total = product(
            lambda cy: rx[j, cy],
            lambda cc: joined(lambda k: s_v[k, cc * 2:cc * 2 + 2].reshape(2 * tokens, strip)),
            s_hbm.shape[1],
        )
        own_part[j, 0] = total[:part_rows]
        own_part[j, 1] = total[part_rows:]
        px_send[j], px_scale[j] = encode(own_part[j, 1 - wide])
        remote(px_scale.at[j], px_rscale.at[j], px_send_sem.at[3], px_recv_sem.at[j, 1], x_peer).start()
        remote(px_send.at[j], px_recv.at[j], px_send_sem.at[2], px_recv_sem.at[j, 0], x_peer).start()

    def gather(j):
        n, h = 1 + j // HALVES, j % HALVES
        received(px_recv.at[j], px_recv_sem.at[j, 0])
        received(px_rscale.at[j], px_recv_sem.at[j, 1])
        value = own_part[j, wide] + decoded(px_recv[j], px_rscale[j])
        if n == deep - 1:
            q[h] = value
            return
        q_send[j], q_scale[j] = encode(value)
        there = at(plane(n), wide, core, y)
        remote(q_scale.at[j], zr_scale.at[z, h], z_send_sem.at[3], z_recv_sem.at[z, 1], there).start()
        remote(q_send.at[j], zr.at[z, h], z_send_sem.at[2], z_recv_sem.at[z, 0], there).start()

    @pl.when(jnp.logical_and(z > 0, z < deep - 2))
    def _():
        pl.semaphore_wait(hello.at[0], 1)
        pl.semaphore_signal(hello.at[0], inc=1, device_id=below, device_id_type=MESH)

    @pl.when(jnp.logical_and(z > 1, z < deep - 1))
    def _():
        pl.semaphore_wait(hello.at[1], 1)
        pl.semaphore_signal(hello.at[1], inc=1, device_id=above, device_id_type=MESH)

    forward_strip(0)
    strip_here(0)
    received(lead_rx.at[0:3], x_recv_sem.at[pieces])
    lead_partial(0)
    forward_strip(1)
    for k in range(1, STRIPS - 1):
        forward_strip(k + 1)
        strip_here(k)
        lead_partial(k)

    @pl.when(z == 0)
    def _():
        pl.semaphore_wait(hello.at[0], 1)

    @pl.when(z == deep - 1)
    def _():
        pl.semaphore_wait(hello.at[1], 1)

    lead_gather(0)
    strip_here(STRIPS - 1)
    lead_partial(STRIPS - 1)

    steps = [functools.partial(lead_gather, k) for k in range(1, STRIPS)]
    steps += [functools.partial(gather, j) for j in range(pieces)]
    for j in range(pieces):
        partial(j)
        if j == GRAD_AFTER:
            other_grad()
        if j >= LAG:
            steps.pop(0)()
    for step in steps:
        step()

    sent(s_v.at[:, 0:3], s_send_sem)
    sent(lead_tx.at[0:3], x_send_sem.at[0])
    sent(tx.at[:, 0:3], x_send_sem.at[1])
    for slot, ref in enumerate((lead_send, lead_scale, px_send, px_scale)):
        sent(ref, px_send_sem.at[slot])

    for n in range(deep - 1):
        source = jnp.where(n < z, n, n + 1)
        received(zr.at[source], z_recv_sem.at[source, 0])
        received(zr_scale.at[source], z_recv_sem.at[source, 1])

    received(ig_send, ig_recv_sem)
    for slot, ref in enumerate((lead_q, lead_qscale, q_send, q_scale)):
        sent(ref, z_send_sem.at[slot])
    sent(ig_send, ig_send_sem)


def write_out(ig_ref, q, zr, zr_scale, ig_hbm, wg_hbm, wg_ref, sems):
    ig_copy = pltpu.make_async_copy(ig_ref, ig_hbm, sems.at[0])
    wg_copy = pltpu.make_async_copy(wg_ref, wg_hbm, sems.at[1])
    ig_copy.start()
    part_rows = q.shape[1]
    for h in range(q.shape[0]):
        total = q[h]
        for source in range(zr.shape[0]):
            total = total + decoded(zr[source, h], zr_scale[source, h])
        wg_ref[h * part_rows:(h + 1) * part_rows, :] = total
    wg_copy.start()
    ig_copy.wait()
    wg_copy.wait()


def kernel_shards(deep, rows, x, s, w, mask, plist):
    tokens, width = x.shape
    values = s.shape[1]
    f32, bf16, i16 = jnp.float32, jnp.bfloat16, jnp.int16
    dma = pltpu.SemaphoreType.DMA
    anywhere = pl.BlockSpec(memory_space=pl.ANY)
    part_rows, pieces, strip = rows // HALVES, (deep - 1) * HALVES, values // STRIPS
    on_chip = pl.pallas_call(
        functools.partial(kernel, deep),
        out_shape=(
            pltpu.VMEM((tokens, width), bf16),
            pltpu.VMEM((HALVES, part_rows, values), f32),
            pltpu.VMEM((deep, HALVES, part_rows, values), i16),
            pltpu.VMEM((deep, HALVES, 1, values), f32),
        ),
        in_specs=[anywhere] * 5,
        out_specs=(pl.BlockSpec(memory_space=pltpu.VMEM),) * 4,
        scratch_shapes=[
            pltpu.SMEM(mask.shape, jnp.int32),
            pltpu.SMEM(plist.shape, jnp.int32),
            pltpu.VMEM((tokens, width), bf16),
            pltpu.VMEM((STRIPS, CORES * 2, tokens, strip), bf16),
            pltpu.VMEM(w.shape, bf16),
            pltpu.VMEM((CORES * 2, WIDE * rows, tokens), bf16),
            pltpu.VMEM((CORES * 2, WIDE * rows, tokens), bf16),
            pltpu.VMEM((pieces, CORES * 2, WIDE * part_rows, tokens), bf16),
            pltpu.VMEM((pieces, CORES * 2, WIDE * part_rows, tokens), bf16),
            pltpu.VMEM((STRIPS, WIDE, rows, strip), f32),
            pltpu.VMEM((STRIPS, rows, strip), i16),
            pltpu.VMEM((STRIPS, 1, strip), f32),
            pltpu.VMEM((STRIPS, rows, strip), i16),
            pltpu.VMEM((STRIPS, 1, strip), f32),
            pltpu.VMEM((STRIPS, HALVES, part_rows, strip), i16),
            pltpu.VMEM((STRIPS, HALVES, 1, strip), f32),
            pltpu.VMEM((pieces, WIDE, part_rows, values), f32),
            pltpu.VMEM((pieces, part_rows, values), i16),
            pltpu.VMEM((pieces, 1, values), f32),
            pltpu.VMEM((pieces, part_rows, values), i16),
            pltpu.VMEM((pieces, 1, values), f32),
            pltpu.VMEM((pieces - HALVES, part_rows, values), i16),
            pltpu.VMEM((pieces - HALVES, 1, values), f32),
            pltpu.VMEM((tokens, w.shape[0]), bf16),
            dma((5,)), dma, dma((STRIPS, 2)), dma((2,)), dma((pieces + 1,)),
            dma((4,)), dma((STRIPS, 2)), dma((pieces, 2)), dma((4,)), dma((deep, 2)), dma, dma,
            pltpu.SemaphoreType.REGULAR((2,)),
        ],
        compiler_params=pltpu.CompilerParams(collective_id=0, has_side_effects=True),
    )(mask, plist, x, s, w)
    return pl.pallas_call(
        write_out,
        out_shape=(
            jax.ShapeDtypeStruct((tokens, width), bf16),
            jax.ShapeDtypeStruct((rows, values), f32),
        ),
        in_specs=[pl.BlockSpec(memory_space=pltpu.VMEM)] * 4,
        out_specs=(anywhere,) * 2,
        scratch_shapes=[pltpu.VMEM((rows, values), f32), dma((2,))],
        compiler_params=pltpu.CompilerParams(vmem_limit_bytes=SMALL),
    )(*(pltpu.with_memory_space_constraint(part, pltpu.VMEM) for part in on_chip))


def solution(mesh):
    outer, inner = mesh.shape["grp"], mesh.shape["fsdp"]

    def shards(x, s, w, mask, plist):
        rows = x.shape[1] // (outer * inner)
        if inner == 2 and outer % (CORES * WIDE) == 0 and outer // (CORES * WIDE) >= 4 and rows % (16 * HALVES) == 0 and x.shape[0] % 128 == 0 and s.shape[1] % (128 * STRIPS) == 0:
            return tuple(kernel_shards(outer // (CORES * WIDE), rows, x, s, w, mask, plist))
        return collective_shards(x, s, w, mask, plist)

    in_specs = (P(("grp", "fsdp"), None), P(("grp", "fsdp"), None), P("fsdp", None), P(), P())
    out_specs = (P(("grp", "fsdp"), None), P(("grp", "fsdp"), None))
    return jax.shard_map(shards, mesh=mesh, in_specs=in_specs, out_specs=out_specs, check_vma=False)
```

```python
import functools

import jax
import jax.numpy as jnp
from jax import lax
from jax.experimental import pallas as pl
from jax.experimental.pallas import tpu as pltpu
from jax.sharding import PartitionSpec as P

MESH = pl.DeviceIdType.MESH
CORES = 2
WIDE = 2
HALVES = 2
STRIPS = 4
LAG = 1
GRAD_AFTER = 1
ORDERS = {4: ((3, 2, 1), (0, 3, 2), (0, 3, 1), (0, 1, 2))}
SMALL = 1 << 21
SHARES = 4
STEPS = 32766.0
TINY = 1e-33


def collective_shards(
    normalized_inputs,
    output_sensitivity,
    projection_weights,
    completion_mask,
    replica_partition_list,
):
    replica_index = lax.axis_index("grp")
    selected_replica = lax.iota(jnp.int32, completion_mask.shape[0]) == replica_index
    assigned_piece = jnp.sum(jnp.where(selected_replica, replica_partition_list, 0))
    finished_indicator = jnp.sum(jnp.where(selected_replica, completion_mask, 0))
    finisher_tally = jnp.sum(
        jnp.where(replica_partition_list == assigned_piece, completion_mask, 0)
    )
    living_float = finished_indicator.astype(jnp.float32)
    decode_sum = living_float / (finisher_tally.astype(jnp.float32) + 1.0 - living_float)
    tokens_here = normalized_inputs.shape[0]
    model_width = normalized_inputs.shape[1]
    inner_size = lax.axis_size("fsdp")
    outer_size = lax.axis_size("grp")
    input_grad = lax.dot_general(
        output_sensitivity,
        lax.all_gather(projection_weights, "fsdp", axis=0, tiled=True),
        (((1,), (1,)), ((), ())),
        preferred_element_type=jnp.float32,
    ).astype(jnp.bfloat16)
    owner_rows = model_width // (outer_size * inner_size)
    reordered = normalized_inputs.reshape(tokens_here, outer_size, inner_size, owner_rows)
    reordered = reordered.transpose(0, 2, 1, 3).reshape(tokens_here, model_width)
    column_block = lax.all_to_all(reordered, "fsdp", split_axis=1, concat_axis=0, tiled=True)
    group_block = lax.dot_general(
        column_block,
        lax.all_gather(output_sensitivity, "fsdp", axis=0, tiled=True),
        (((0,), (0,)), ((), ())),
        preferred_element_type=jnp.float32,
    )
    weight_grad = lax.psum_scatter(decode_sum * group_block, "grp", scatter_dimension=0, tiled=True)
    return (input_grad, weight_grad)


def encode(value):
    top = jnp.maximum(jnp.max(jnp.abs(value), axis=0, keepdims=True), TINY)
    coded = jnp.round(value * (STEPS / top)).astype(jnp.int32).astype(jnp.int16)
    return coded, top * (1.0 / STEPS)


def decoded(coded, step):
    return coded.astype(jnp.int32).astype(jnp.float32) * step


def kernel(
    deep,
    mask_hbm, list_hbm, x_hbm, s_hbm, w_hbm,
    ig_ref, q, zr, zr_scale,
    mask_ref, list_ref,
    x_v, s_v, w_v, lead_tx, lead_rx, tx, rx,
    lead_part, lead_send, lead_scale, lead_recv, lead_rscale, lead_q, lead_qscale,
    own_part, px_send, px_scale, px_recv, px_rscale, q_send, q_scale, ig_send,
    load_sem, s_send_sem, s_recv_sem, x_send_sem, x_recv_sem,
    px_send_sem, lead_recv_sem, px_recv_sem, z_send_sem, z_recv_sem, ig_send_sem, ig_recv_sem, hello,
):
    grp = lax.axis_index("grp")
    y = lax.axis_index("fsdp")
    core = lax.rem(grp, CORES)
    wide = lax.rem(grp // CORES, WIDE)
    z = grp // (CORES * WIDE)
    oy, oc = 1 - y, 1 - core
    tokens = s_hbm.shape[0]
    groups = mask_ref.shape[0]
    rows = q.shape[0] * q.shape[1]
    half = w_hbm.shape[0]
    part_tokens = tokens // 2
    part_rows = rows // HALVES
    pieces = (deep - 1) * HALVES
    strip = s_hbm.shape[1] // STRIPS

    def at(zz, xx, cc, yy):
        return ((zz * WIDE + xx) * CORES + cc, yy)

    def remote(src, dst, send, recv, device):
        return pltpu.make_async_remote_copy(
            src_ref=src, dst_ref=dst, send_sem=send, recv_sem=recv,
            device_id=device, device_id_type=MESH,
        )

    y_peer = at(z, wide, core, oy)
    y_cross = at(z, wide, oc, oy)
    sibling = at(z, wide, oc, y)
    x_peer = at(z, 1 - wide, core, y)
    below = at(lax.rem(z + deep - 1, deep), wide, core, y)
    above = at(lax.rem(z + 1, deep), wide, core, y)
    me = core * 2 + y
    from_y = core * 2 + oy
    from_cross = oc * 2 + oy
    from_sib = oc * 2 + y

    barrier = pltpu.get_barrier_semaphore()
    partners = [y_peer, y_cross, sibling, x_peer]
    for partner in partners:
        pl.semaphore_signal(barrier, inc=1, device_id=partner, device_id_type=MESH)

    @pl.when(z > 0)
    def _():
        pl.semaphore_signal(barrier, inc=1, device_id=below, device_id_type=MESH)

    @pl.when(z < deep - 1)
    def _():
        pl.semaphore_signal(barrier, inc=1, device_id=above, device_id_type=MESH)

    load_x = pltpu.make_async_copy(x_hbm, x_v, load_sem.at[0])
    load_w = pltpu.make_async_copy(w_hbm, w_v, load_sem.at[2])
    load_mask = pltpu.make_async_copy(mask_hbm, mask_ref, load_sem.at[3])
    load_list = pltpu.make_async_copy(list_hbm, list_ref, load_sem.at[4])
    columns = [pl.ds(k * strip, strip) for k in range(STRIPS)]
    load_x.start()
    for k in range(STRIPS):
        pltpu.make_async_copy(s_hbm.at[:, columns[k]], s_v.at[k, me], load_sem.at[1]).start()
    load_w.start()
    load_mask.start()
    load_list.start()

    first, second = pl.ds(0, part_tokens), pl.ds(part_tokens, part_tokens)
    def received(ref, sem):
        remote(ref, ref, sem, sem, sibling).wait_recv()

    def sent(ref, sem):
        remote(ref, ref, sem, sem, sibling).wait_send()

    def send_strip(k):
        own = s_v.at[k, me]
        remote(s_hbm.at[first, columns[k]], own.at[first], s_send_sem, s_recv_sem.at[k, 0], y_peer).start()
        remote(s_hbm.at[second, columns[k]], own.at[second], s_send_sem, s_recv_sem.at[k, 0], y_cross).start()
        remote(s_hbm.at[:, columns[k]], own, s_send_sem, s_recv_sem.at[k, 1], sibling).start()

    def forward_strip(k):
        received(s_v.at[k, me], s_recv_sem.at[k, 0])
        for landed in (s_v.at[k, from_y, first], s_v.at[k, from_cross, second]):
            remote(landed, landed, s_send_sem, s_recv_sem.at[k, 1], sibling).start()

    def strip_here(k):
        received(s_v.at[k, 0:2], s_recv_sem.at[k, 1])

    @pl.when(jnp.logical_and(z > 0, z < deep - 1))
    def _():
        pl.semaphore_wait(barrier, len(partners) + 2)

    @pl.when(jnp.logical_or(z == 0, z == deep - 1))
    def _():
        pl.semaphore_wait(barrier, len(partners) + 1)

    send_strip(0)

    @pl.when(z == deep - 2)
    def _():
        pl.semaphore_signal(hello.at[0], inc=1, device_id=below, device_id_type=MESH)

    @pl.when(z == 1)
    def _():
        pl.semaphore_signal(hello.at[1], inc=1, device_id=above, device_id_type=MESH)

    span = WIDE * CORES * 2 * rows

    orders = ORDERS.get(deep) or [[p for p in range(deep) if p != own] for own in range(deep)]

    def plane(n):
        if n == deep - 1:
            return z
        there = jnp.int32(0)
        for own in range(deep):
            there = jnp.where(z == own, orders[own][n], there)
        return there

    def turn(n):
        part = x_v[:, pl.ds(pl.multiple_of(plane(n) * span, span), span)].T
        for xx in range(WIDE):
            for cy in range(CORES * 2):
                start = (xx * CORES * 2 + cy) * rows
                if n == 0:
                    lead_tx[cy, xx * rows:(xx + 1) * rows, :] = part[start:start + rows, :]
                    continue
                for h in range(HALVES):
                    top = start + h * part_rows
                    tx[(n - 1) * HALVES + h, cy, xx * part_rows:(xx + 1) * part_rows, :] = part[top:top + part_rows, :]

    there_of = ((y_peer, from_y), (y_cross, from_cross), (sibling, from_sib))
    load_x.wait()
    turn(0)
    for device, there in there_of:
        remote(lead_tx.at[there], lead_rx.at[me], x_send_sem.at[0], x_recv_sem.at[pieces], device).start()
    for k in range(1, STRIPS):
        send_strip(k)
    lead_rx[me] = lead_tx[me]
    for n in range(1, deep):
        turn(n)
        for j in range((n - 1) * HALVES, n * HALVES):
            for device, there in there_of:
                remote(tx.at[j, there], rx.at[j, me], x_send_sem.at[1], x_recv_sem.at[j], device).start()
            rx[j, me] = tx[j, me]

    load_mask.wait()
    load_list.wait()
    scales = []
    for cc in range(CORES):
        here = (z * WIDE + wide) * CORES + cc
        mine = list_ref[here]
        tally = jnp.int32(0)
        for h in range(groups):
            tally = tally + jnp.where(list_ref[h] == mine, mask_ref[h], 0)
        done = jnp.full((1, s_hbm.shape[1]), mask_ref[here], jnp.int32).astype(jnp.float32)
        total = jnp.full((1, s_hbm.shape[1]), tally, jnp.int32).astype(jnp.float32)
        scales.append(done / (total + 1.0 - done))

    pltpu.make_async_copy(s_v.at[:, me], s_v.at[:, me], load_sem.at[1]).wait()
    load_w.wait()

    def grad(s_block):
        return lax.dot_general(
            s_block, w_v[...], (((1,), (1,)), ((), ())), preferred_element_type=jnp.float32
        ).astype(jnp.bfloat16)

    def joined(part):
        return jnp.concatenate([part(k) for k in range(STRIPS)], axis=1)

    zr[z] = jnp.zeros(zr.shape[1:], zr.dtype)
    zr_scale[z] = jnp.zeros(zr_scale.shape[1:], zr_scale.dtype)

    own_columns = pl.ds(pl.multiple_of(y * half, half), half)
    ig_ref[:, own_columns] = grad(joined(lambda k: s_v[k, me]))

    def other_grad():
        block = [joined(lambda k: s_v[k, from_y, first]), joined(lambda k: s_v[k, from_cross, second])]
        ig_send[...] = grad(jnp.concatenate(block, axis=0))
        for tokens_of, device in ((first, y_peer), (second, y_cross)):
            remote(
                ig_send.at[tokens_of], ig_ref.at[tokens_of, own_columns], ig_send_sem, ig_recv_sem, device
            ).start()

    def product(lefts, rights, width):
        total = None
        for cc in range(CORES):
            left = jnp.concatenate([lefts(cc * 2), lefts(cc * 2 + 1)], axis=1)
            term = scales[cc][:, :width] * jnp.dot(left, rights(cc), preferred_element_type=jnp.float32)
            total = term if total is None else total + term
        return total

    def lead_partial(k):
        total = product(
            lambda cy: lead_rx[cy], lambda cc: s_v[k, cc * 2:cc * 2 + 2].reshape(2 * tokens, strip), strip
        )
        lead_part[k, 0] = total[:rows]
        lead_part[k, 1] = total[rows:]
        lead_send[k], lead_scale[k] = encode(lead_part[k, 1 - wide])
        remote(lead_scale.at[k], lead_rscale.at[k], px_send_sem.at[1], lead_recv_sem.at[k, 1], x_peer).start()
        remote(lead_send.at[k], lead_recv.at[k], px_send_sem.at[0], lead_recv_sem.at[k, 0], x_peer).start()

    def lead_gather(k):
        received(lead_recv.at[k], lead_recv_sem.at[k, 0])
        received(lead_rscale.at[k], lead_recv_sem.at[k, 1])
        coded, scale = encode(lead_part[k, wide] + decoded(lead_recv[k], lead_rscale[k]))
        for h in range(HALVES):
            lead_q[k, h] = coded[h * part_rows:(h + 1) * part_rows]
            lead_qscale[k, h] = scale
        there = at(plane(0), wide, core, y)
        for slot, (src, dst) in ((1, (lead_qscale, zr_scale)), (0, (lead_q, zr))):
            remote(
                src.at[k], dst.at[z, :, :, columns[k]], z_send_sem.at[slot], z_recv_sem.at[z, slot], there
            ).start()

    def partial(j):
        received(rx.at[j, 0:3], x_recv_sem.at[j])
        total = product(
            lambda cy: rx[j, cy],
            lambda cc: joined(lambda k: s_v[k, cc * 2:cc * 2 + 2].reshape(2 * tokens, strip)),
            s_hbm.shape[1],
        )
        own_part[j, 0] = total[:part_rows]
        own_part[j, 1] = total[part_rows:]
        px_send[j], px_scale[j] = encode(own_part[j, 1 - wide])
        remote(px_scale.at[j], px_rscale.at[j], px_send_sem.at[3], px_recv_sem.at[j, 1], x_peer).start()
        remote(px_send.at[j], px_recv.at[j], px_send_sem.at[2], px_recv_sem.at[j, 0], x_peer).start()

    def gather(j):
        n, h = 1 + j // HALVES, j % HALVES
        received(px_recv.at[j], px_recv_sem.at[j, 0])
        received(px_rscale.at[j], px_recv_sem.at[j, 1])
        value = own_part[j, wide] + decoded(px_recv[j], px_rscale[j])
        if n == deep - 1:
            q[h] = value
            return
        q_send[j], q_scale[j] = encode(value)
        there = at(plane(n), wide, core, y)
        remote(q_scale.at[j], zr_scale.at[z, h], z_send_sem.at[3], z_recv_sem.at[z, 1], there).start()
        remote(q_send.at[j], zr.at[z, h], z_send_sem.at[2], z_recv_sem.at[z, 0], there).start()

    @pl.when(jnp.logical_and(z > 0, z < deep - 2))
    def _():
        pl.semaphore_wait(hello.at[0], 1)
        pl.semaphore_signal(hello.at[0], inc=1, device_id=below, device_id_type=MESH)

    @pl.when(jnp.logical_and(z > 1, z < deep - 1))
    def _():
        pl.semaphore_wait(hello.at[1], 1)
        pl.semaphore_signal(hello.at[1], inc=1, device_id=above, device_id_type=MESH)

    forward_strip(0)
    strip_here(0)
    received(lead_rx.at[0:3], x_recv_sem.at[pieces])
    lead_partial(0)
    forward_strip(1)
    for k in range(1, STRIPS - 1):
        forward_strip(k + 1)
        strip_here(k)
        lead_partial(k)

    @pl.when(z == 0)
    def _():
        pl.semaphore_wait(hello.at[0], 1)

    @pl.when(z == deep - 1)
    def _():
        pl.semaphore_wait(hello.at[1], 1)

    lead_gather(0)
    strip_here(STRIPS - 1)
    lead_partial(STRIPS - 1)

    steps = [functools.partial(lead_gather, k) for k in range(1, STRIPS)]
    steps += [functools.partial(gather, j) for j in range(pieces)]
    for j in range(pieces):
        partial(j)
        if j == GRAD_AFTER:
            other_grad()
        if j >= LAG:
            steps.pop(0)()
    for step in steps:
        step()

    sent(s_v.at[:, 0:3], s_send_sem)
    sent(lead_tx.at[0:3], x_send_sem.at[0])
    sent(tx.at[:, 0:3], x_send_sem.at[1])
    for slot, ref in enumerate((lead_send, lead_scale, px_send, px_scale)):
        sent(ref, px_send_sem.at[slot])

    for n in range(deep - 1):
        source = jnp.where(n < z, n, n + 1)
        received(zr.at[source], z_recv_sem.at[source, 0])
        received(zr_scale.at[source], z_recv_sem.at[source, 1])

    received(ig_send, ig_recv_sem)
    for slot, ref in enumerate((lead_q, lead_qscale, q_send, q_scale)):
        sent(ref, z_send_sem.at[slot])
    sent(ig_send, ig_send_sem)


def write_out(ig_ref, q, zr, zr_scale, ig_hbm, wg_hbm, wg_ref, sems):
    ig_copy = pltpu.make_async_copy(ig_ref, ig_hbm, sems.at[0])
    wg_copy = pltpu.make_async_copy(wg_ref, wg_hbm, sems.at[1])
    share = ig_ref.shape[0] // SHARES
    for k in range(SHARES):
        rows_of = pl.ds(k * share, share)
        pltpu.make_async_copy(ig_ref.at[rows_of], ig_hbm.at[rows_of], sems.at[0]).start()
    part_rows = q.shape[1]
    for h in range(q.shape[0]):
        total = q[h]
        for source in range(zr.shape[0]):
            total = total + decoded(zr[source, h], zr_scale[source, h])
        wg_ref[h * part_rows:(h + 1) * part_rows, :] = total
    wg_copy.start()
    ig_copy.wait()
    wg_copy.wait()


def kernel_shards(deep, rows, x, s, w, mask, plist):
    tokens, width = x.shape
    values = s.shape[1]
    f32, bf16, i16 = jnp.float32, jnp.bfloat16, jnp.int16
    dma = pltpu.SemaphoreType.DMA
    anywhere = pl.BlockSpec(memory_space=pl.ANY)
    part_rows, pieces, strip = rows // HALVES, (deep - 1) * HALVES, values // STRIPS
    on_chip = pl.pallas_call(
        functools.partial(kernel, deep),
        out_shape=(
            pltpu.VMEM((tokens, width), bf16),
            pltpu.VMEM((HALVES, part_rows, values), f32),
            pltpu.VMEM((deep, HALVES, part_rows, values), i16),
            pltpu.VMEM((deep, HALVES, 1, values), f32),
        ),
        in_specs=[anywhere] * 5,
        out_specs=(pl.BlockSpec(memory_space=pltpu.VMEM),) * 4,
        scratch_shapes=[
            pltpu.SMEM(mask.shape, jnp.int32),
            pltpu.SMEM(plist.shape, jnp.int32),
            pltpu.VMEM((tokens, width), bf16),
            pltpu.VMEM((STRIPS, CORES * 2, tokens, strip), bf16),
            pltpu.VMEM(w.shape, bf16),
            pltpu.VMEM((CORES * 2, WIDE * rows, tokens), bf16),
            pltpu.VMEM((CORES * 2, WIDE * rows, tokens), bf16),
            pltpu.VMEM((pieces, CORES * 2, WIDE * part_rows, tokens), bf16),
            pltpu.VMEM((pieces, CORES * 2, WIDE * part_rows, tokens), bf16),
            pltpu.VMEM((STRIPS, WIDE, rows, strip), f32),
            pltpu.VMEM((STRIPS, rows, strip), i16),
            pltpu.VMEM((STRIPS, 1, strip), f32),
            pltpu.VMEM((STRIPS, rows, strip), i16),
            pltpu.VMEM((STRIPS, 1, strip), f32),
            pltpu.VMEM((STRIPS, HALVES, part_rows, strip), i16),
            pltpu.VMEM((STRIPS, HALVES, 1, strip), f32),
            pltpu.VMEM((pieces, WIDE, part_rows, values), f32),
            pltpu.VMEM((pieces, part_rows, values), i16),
            pltpu.VMEM((pieces, 1, values), f32),
            pltpu.VMEM((pieces, part_rows, values), i16),
            pltpu.VMEM((pieces, 1, values), f32),
            pltpu.VMEM((pieces - HALVES, part_rows, values), i16),
            pltpu.VMEM((pieces - HALVES, 1, values), f32),
            pltpu.VMEM((tokens, w.shape[0]), bf16),
            dma((5,)), dma, dma((STRIPS, 2)), dma((2,)), dma((pieces + 1,)),
            dma((4,)), dma((STRIPS, 2)), dma((pieces, 2)), dma((4,)), dma((deep, 2)), dma, dma,
            pltpu.SemaphoreType.REGULAR((2,)),
        ],
        compiler_params=pltpu.CompilerParams(collective_id=0, has_side_effects=True),
    )(mask, plist, x, s, w)
    return pl.pallas_call(
        write_out,
        out_shape=(
            jax.ShapeDtypeStruct((tokens, width), bf16),
            jax.ShapeDtypeStruct((rows, values), f32),
        ),
        in_specs=[pl.BlockSpec(memory_space=pltpu.VMEM)] * 4,
        out_specs=(anywhere,) * 2,
        scratch_shapes=[pltpu.VMEM((rows, values), f32), dma((2,))],
        compiler_params=pltpu.CompilerParams(vmem_limit_bytes=SMALL),
    )(*(pltpu.with_memory_space_constraint(part, pltpu.VMEM) for part in on_chip))


def solution(mesh):
    outer, inner = mesh.shape["grp"], mesh.shape["fsdp"]

    def shards(x, s, w, mask, plist):
        rows = x.shape[1] // (outer * inner)
        if inner == 2 and outer % (CORES * WIDE) == 0 and outer // (CORES * WIDE) >= 4 and rows % (16 * HALVES) == 0 and x.shape[0] % 128 == 0 and s.shape[1] % (128 * STRIPS) == 0:
            return tuple(kernel_shards(outer // (CORES * WIDE), rows, x, s, w, mask, plist))
        return collective_shards(x, s, w, mask, plist)

    in_specs = (P(("grp", "fsdp"), None), P(("grp", "fsdp"), None), P("fsdp", None), P(), P())
    out_specs = (P(("grp", "fsdp"), None), P(("grp", "fsdp"), None))
    return jax.shard_map(shards, mesh=mesh, in_specs=in_specs, out_specs=out_specs, check_vma=False)
```
